256 devices in a mesh: outer: 8 (over y, core), inner: 32 (over x, z).
Axes of the slice: x: 4, y: 4, z: 8, core: 2. Of those that a mesh axis runs over, the one named last changes fastest.
Arguments:
- amplitudes: float32 [2, 67108864], P(None, ('outer', 'inner')), may hold values from -200 to 200
Outputs:
- transformed: float32 [2, 67108864], P(None, ('outer', 'inner'))
- checks: float32 [3], replicated
The draws below stay inside these ranges and needn't reach their ends.
All inputs are finite; a program needn't handle non-finite values.
Results may differ from the reference program's by a relative error of at most 0.00007.
Values sent between devices are 32-bit elements; how exact they have to be, the bound alone decides.
A program may use at most 64 MiB of HBM per device.

```python
import math
import jax
import jax.numpy as jnp
from jax import lax

AMP_DEV = 262144
WINDOW = 9
DEVICES = 256


def draw_amplitudes(key, part):
    total_len = AMP_DEV * DEVICES
    first, second = jax.random.split(key, 2)
    position = jnp.arange(total_len, dtype=jnp.int32)
    device_pos = (position // AMP_DEV).astype(jnp.float32) / max(DEVICES - 1, 1)
    cell_scale = jnp.exp(jax.random.uniform(second, (total_len,), jnp.float32) * math.log(10.0))
    values = jnp.clip(jax.random.normal(first, (2, total_len), jnp.float32), -5.0, 5.0)
    ramp = 3.0 ** device_pos
    return values * ramp * cell_scale / 3.0


def setup_inputs(seed: int = 0) -> dict:
    streams_of = jax.random.split(jax.random.key(seed), 2)
    return {
        "amplitudes": draw_amplitudes(jax.random.fold_in(streams_of[1], 71), 0),
    }


def bit_reverse_table(count):
    result = []
    for value in range(2 ** count):
        flipped = 0
        for bit_pos in range(count):
            flipped = flipped | (value >> bit_pos & 1) << count - 1 - bit_pos
        result.append(flipped)
    return jnp.array(result, dtype=jnp.int32)

def reference(amplitudes):
    columns = 2 ** WINDOW
    total_len = AMP_DEV * DEVICES
    qubits = total_len.bit_length() - 1
    complex_amp = lax.complex(amplitudes[0], amplitudes[1]).reshape(-1, columns)
    spectrum = jnp.fft.ifft(complex_amp, axis=-1) * math.sqrt(columns)
    windowed = spectrum[:, bit_reverse_table(WINDOW)].reshape(-1)
    stacked = jnp.stack([jnp.real(windowed), jnp.imag(windowed)])
    expanded = stacked.reshape((2,) + (2,) * qubits)
    reversed_field = jnp.transpose(expanded, [0] + list(range(qubits, 0, -1))).reshape(2, total_len)
    mean_square = jnp.sum(reversed_field * reversed_field) / total_len
    factor = lax.rsqrt(mean_square + 1e-06)
    transformed = reversed_field * factor
    angles = jnp.arange(total_len, dtype=jnp.int32).astype(jnp.float32) * (2.0 * math.pi / total_len)
    cosine = jnp.cos(angles)
    sine = jnp.sin(angles)
    scaled = 1.0 / math.sqrt(total_len)
    phase_real = jnp.sum(transformed[0] * cosine + transformed[1] * sine) * scaled
    phase_imag = jnp.sum(transformed[1] * cosine - transformed[0] * sine) * scaled
    return (transformed, jnp.stack([mean_square, phase_real, phase_imag]))
```

```python
import functools
import math

import jax
import jax.numpy as jnp
import numpy as np
from jax import lax
from jax.experimental import pallas as pl
from jax.experimental.pallas import tpu as pltpu
from jax.sharding import PartitionSpec as P

MESH = pl.DeviceIdType.MESH
AXES = ("outer", "inner")
AMP_DEV = 262144
DEVICES = 256
TOTAL = AMP_DEV * DEVICES
WINDOW = 512
ROWS = AMP_DEV // WINDOW
PITCH = 520


def dft_tables():
    e = np.arange(128)
    angle = 2.0 * np.pi * ((e[:, None] * e[None, :]) % 128) / 128.0
    cosine = np.cos(angle) / math.sqrt(WINDOW)
    sine = np.sin(angle) / math.sqrt(WINDOW)
    table = np.block([[cosine, -sine], [sine, cosine]]).astype(np.float32)
    high = table.astype(jnp.bfloat16)
    low = (table - high.astype(np.float32)).astype(jnp.bfloat16)
    twiddle = np.zeros((8, 128), np.float32)
    for g in (1, 2, 3):
        twiddle[2 * g - 2] = np.cos(2.0 * np.pi * g * e / WINDOW)
        twiddle[2 * g - 1] = np.sin(2.0 * np.pi * g * e / WINDOW)
    return high, low, twiddle


def reverse_bits(value, count):
    result = 0
    for bit in range(count):
        result = result + (value // 2**bit) % 2 * 2 ** (count - 1 - bit)
    return result


def exchange_kernel(
    x_ref, high_ref, low_ref, twiddle_ref, recv_ref, sums_ref,
    a_ref, bh_ref, bl_ref, send_ref, zsum_ref, xsum_ref, ysum_ref, csum_ref,
    load_sem, send_sem, recv_sem, round_sem, sum_send_sem, sum_recv_sem,
):
    outer, inner = lax.axis_index("outer"), lax.axis_index("inner")
    y, c, x, z = outer // 2, outer % 2, inner // 8, inner % 8
    me = outer * 32 + inner
    slot = reverse_bits(me, 8)

    def device(dy, dc, dx, dz):
        return ((y + dy) % 4 * 2 + (c + dc) % 2, (x + dx) % 4 * 8 + (z + dz) % 8)

    z_peers = [device(0, 0, 0, d) for d in range(1, 8)]
    x_peers = [device(0, 0, d, 0) for d in range(1, 4)]
    y_peers = [device(d, 0, 0, 0) for d in range(1, 4)]
    c_peers = [device(0, 1, 0, 0)]

    barrier = pltpu.get_barrier_semaphore()
    for peer in z_peers + x_peers + y_peers + c_peers:
        pl.semaphore_signal(barrier, inc=1, device_id=peer, device_id_type=MESH)

    loads = []
    for top in range(8):
        load = pltpu.make_async_copy(
            x_ref.at[pl.ds(512 * top, 512)],
            a_ref.at[pl.ds(PITCH * reverse_bits(top, 3), 512)],
            load_sem.at[top],
        )
        load.start()
        loads.append(load)
    for load in loads:
        load.wait()

    twiddles = [
        (twiddle_ref[pl.ds(2 * g - 2, 1), :], twiddle_ref[pl.ds(2 * g - 1, 1), :]) for g in (1, 2, 3)
    ]
    step = 2.0 * math.pi * 2048 / TOTAL
    cos_step, sin_step = math.cos(step), math.sin(step)

    def spread(turn, carry):
        squares, phase_real, phase_imag = carry
        h = 31 - turn
        row = reverse_bits(h, 5)
        parts = [
            [a_ref[pl.ds((row + 32 * b) * 8 + q, 8, stride=PITCH), :] for q in range(8)] for b in range(2)
        ]
        for b in (1, 0):
            phase_real, phase_imag = (
                phase_real * cos_step + phase_imag * sin_step + parts[b][0],
                phase_imag * cos_step - phase_real * sin_step + parts[b][1],
            )
            for q in range(8):
                squares = squares + parts[b][q] * parts[b][q]
        v = [jnp.concatenate([parts[0][q], parts[1][q]], 0) for q in range(8)]
        real, imag = v[0::2], v[1::2]
        s02r, s02i = real[0] + real[2], imag[0] + imag[2]
        d02r, d02i = real[0] - real[2], imag[0] - imag[2]
        s13r, s13i = real[1] + real[3], imag[1] + imag[3]
        d13r, d13i = real[1] - real[3], imag[1] - imag[3]
        u = [
            (s02r + s13r, s02i + s13i),
            (d02r - d13i, d02i + d13r),
            (s02r - s13r, s02i - s13i),
            (d02r + d13i, d02i - d13r),
        ]
        rows = pl.ds(pl.multiple_of(h * 16, 16), 16)
        for g in range(4):
            ur, ui = u[g]
            if g:
                cosine, sine = twiddles[g - 1]
                ur, ui = ur * cosine - ui * sine, ur * sine + ui * cosine
            for s, value in ((0, ur), (1, ui)):
                high = value.astype(jnp.bfloat16)
                low = (value - high.astype(jnp.float32)).astype(jnp.bfloat16)
                bh_ref[g, rows, 128 * s : 128 * s + 128] = high
                bl_ref[g, rows, 128 * s : 128 * s + 128] = low
        return squares, phase_real, phase_imag

    zero = jnp.zeros((8, 128), jnp.float32)
    squares, phase_real, phase_imag = lax.fori_loop(0, 32, spread, (zero, zero, zero))

    high, low = high_ref[...], low_ref[...]

    def transform(step, _):
        g, part = step // 2, step % 2
        rows = pl.ds(pl.multiple_of(part * 256, 256), 256)
        bh, bl = bh_ref[g, rows, :], bl_ref[g, rows, :]
        dims = (((1,), (1,)), ((), ()))
        out = (
            lax.dot_general(high, bh, dims, preferred_element_type=jnp.float32)
            + lax.dot_general(high, bl, dims, preferred_element_type=jnp.float32)
            + lax.dot_general(low, bh, dims, preferred_element_type=jnp.float32)
        )
        for s in range(2):
            for k in range(2):
                first = g // 2 * 1024 + (part * 2 + k) * 2 + s
                send_ref[g % 2, pl.ds(first, 128, stride=8), :] = out[
                    128 * s : 128 * s + 128, 128 * k : 128 * k + 128
                ]
        return 0

    lax.fori_loop(0, 8, transform, 0)

    lane = lax.broadcasted_iota(jnp.int32, (8, 128), 1)
    sub = lax.broadcasted_iota(jnp.int32, (8, 128), 0)
    angle = (sub * 256 + slot).astype(jnp.float32) * (2.0 * math.pi / TOTAL)
    cosine, sine = jnp.cos(angle), jnp.sin(angle)
    turned_real = jnp.where(lane == 1, phase_real * cosine + phase_imag * sine, 0.0)
    turned_imag = jnp.where(lane == 1, phase_imag * cosine - phase_real * sine, 0.0)
    mine = jnp.where(
        sub == 0,
        jnp.sum(squares, 0, keepdims=True),
        jnp.where(
            sub == 1,
            jnp.sum(turned_real, 0, keepdims=True),
            jnp.where(sub == 2, jnp.sum(turned_imag, 0, keepdims=True), 0.0),
        ),
    )

    pl.semaphore_wait(barrier, 14)
    for number, peers in enumerate((x_peers, y_peers, c_peers)):
        for peer in peers:
            pl.semaphore_signal(round_sem.at[number], inc=1, device_id=peer, device_id_type=MESH)
        pl.semaphore_wait(round_sem.at[number], len(peers))

    def copy(peer, source, target, number):
        return pltpu.make_async_remote_copy(
            src_ref=source,
            dst_ref=target,
            send_sem=sum_send_sem.at[number],
            recv_sem=sum_recv_sem.at[number],
            device_id=peer,
            device_id_type=MESH,
        )

    def bulk(peer, at):
        return pltpu.make_async_remote_copy(
            src_ref=send_ref.at[:, pl.ds(pl.multiple_of(at * 8, 8), 8)],
            dst_ref=recv_ref.at[:, pl.ds(pl.multiple_of(slot * 8, 8), 8)],
            send_sem=send_sem,
            recv_sem=recv_sem,
            device_id=peer,
            device_id_type=MESH,
        )

    def send_bulk(first, last):
        def body(t, _):
            dz, dx, dc, dy = t % 8, t // 8 % 4, t // 32 % 2, t // 64
            peer = device(dy, dc, dx, dz)
            target = peer[0] * 32 + peer[1]
            bulk(peer, target % 2 * 128 + target // 2).start()
            return 0

        lax.fori_loop(first, last, body, 0)

    total = mine
    for number, (peers, place, buffer, first) in enumerate((
        (z_peers, z, zsum_ref, 1),
        (x_peers, x, xsum_ref, 64),
        (y_peers, y, ysum_ref, 128),
        (c_peers, c, csum_ref, 192),
    )):
        buffer[place] = total
        for peer in peers:
            copy(peer, buffer.at[place], buffer.at[place], number).start()
        send_bulk(first, 64 * number + 64)
        if number == 0:
            own = pl.multiple_of((me % 2 * 128 + me // 2) * 8, 8)
            recv_ref[:, pl.ds(pl.multiple_of(slot * 8, 8), 8), :] = send_ref[:, pl.ds(own, 8), :]
        n = len(peers)
        done = copy(peers[0], buffer.at[pl.ds(0, n)], buffer.at[pl.ds(0, n)], number)
        done.wait_recv()
        done.wait_send()
        total = buffer[0]
        for i in range(1, n + 1):
            total = total + buffer[i]
    sums_ref[...] = total

    done = pltpu.make_async_remote_copy(
        src_ref=send_ref.at[:, pl.ds(0, 2040)],
        dst_ref=recv_ref.at[:, pl.ds(0, 2040)],
        send_sem=send_sem,
        recv_sem=recv_sem,
        device_id=c_peers[0],
        device_id_type=MESH,
    )
    done.wait_recv()
    done.wait_send()


def place_kernel(recv_ref, sums_ref, out_ref, checks_ref):
    step = pl.program_id(0)
    half, part = step // 4, step % 4
    mean_square = jnp.sum(sums_ref[pl.ds(0, 1), :], axis=1, keepdims=True) / TOTAL
    factor = lax.rsqrt(mean_square + 1e-06)
    for s in range(2):
        for d in range(2):
            block = recv_ref[half, pl.ds(d * 1024 + part * 2 + s, 128, stride=8), :]
            out_ref[pl.ds(d * 2 + s, 128, stride=4), :] = block.T * factor

    @pl.when(step == 0)
    def _():
        scale = factor * (math.sqrt(WINDOW) / math.sqrt(TOTAL))
        checks_ref[0] = mean_square[0, 0]
        for i in (1, 2):
            value = jnp.sum(sums_ref[pl.ds(i, 1), :], axis=1, keepdims=True) * scale
            checks_ref[i] = value[0, 0]


def per_device(amplitudes):
    high, low, twiddle = dft_tables()
    rows = amplitudes.reshape(2, 2048, 128).transpose(1, 0, 2).reshape(4096, 128)
    vmem = pl.BlockSpec(memory_space=pltpu.VMEM)
    recv, sums = pl.pallas_call(
        exchange_kernel,
        out_shape=(
            jax.ShapeDtypeStruct((2, 2048, 128), jnp.float32),
            jax.ShapeDtypeStruct((8, 128), jnp.float32),
        ),
        in_specs=[pl.BlockSpec(memory_space=pl.ANY), vmem, vmem, vmem],
        out_specs=(vmem, vmem),
        scratch_shapes=[
            pltpu.VMEM((8 * PITCH, 128), jnp.float32),
            pltpu.VMEM((4, 512, 256), jnp.bfloat16),
            pltpu.VMEM((4, 512, 256), jnp.bfloat16),
            pltpu.VMEM((2, 2048, 128), jnp.float32),
            pltpu.VMEM((8, 8, 128), jnp.float32),
            pltpu.VMEM((4, 8, 128), jnp.float32),
            pltpu.VMEM((4, 8, 128), jnp.float32),
            pltpu.VMEM((2, 8, 128), jnp.float32),
            pltpu.SemaphoreType.DMA((8,)),
            pltpu.SemaphoreType.DMA,
            pltpu.SemaphoreType.DMA,
            pltpu.SemaphoreType.REGULAR((3,)),
            pltpu.SemaphoreType.DMA((4,)),
            pltpu.SemaphoreType.DMA((4,)),
        ],
        compiler_params=pltpu.CompilerParams(
            collective_id=1, has_side_effects=True, vmem_limit_bytes=24 * 1024 * 1024
        ),
    )(rows, jnp.asarray(high), jnp.asarray(low), jnp.asarray(twiddle))
    placed, checks = pl.pallas_call(
        place_kernel,
        grid=(8,),
        out_shape=(
            jax.ShapeDtypeStruct((4096, 128), jnp.float32),
            jax.ShapeDtypeStruct((3,), jnp.float32),
        ),
        in_specs=[vmem, vmem],
        out_specs=(
            pl.BlockSpec((512, 128), lambda i: (i, 0)),
            pl.BlockSpec(memory_space=pltpu.SMEM),
        ),
        compiler_params=pltpu.CompilerParams(vmem_limit_bytes=16 * 1024 * 1024),
    )(recv, sums)
    transformed = placed.reshape(2048, 2, 128).transpose(1, 0, 2).reshape(2, AMP_DEV)
    return transformed, checks


def solution(mesh):
    return jax.shard_map(
        per_device,
        mesh=mesh,
        in_specs=(P(None, AXES),),
        out_specs=(P(None, AXES), P()),
        check_vma=False,
    )
```

```python
import math

import jax
import jax.numpy as jnp
import numpy as np
from jax import lax
from jax.experimental import pallas as pl
from jax.experimental.pallas import tpu as pltpu
from jax.sharding import PartitionSpec as P

MESH = pl.DeviceIdType.MESH
AXES = ("outer", "inner")
AMP_DEV = 262144
DEVICES = 256
TOTAL = AMP_DEV * DEVICES
WINDOW = 512
PITCH = 520


def dft_tables():
    e = np.arange(128)
    frequency = e % 32 * 4 + e // 32
    angle = 2.0 * np.pi * ((frequency[:, None] * e[None, :]) % 128) / 128.0
    cosine = np.cos(angle) / math.sqrt(WINDOW)
    sine = np.sin(angle) / math.sqrt(WINDOW)
    table = np.block([[cosine, -sine], [sine, cosine]]).astype(np.float32)
    high = table.astype(jnp.bfloat16)
    low = (table - high.astype(np.float32)).astype(jnp.bfloat16)
    twiddle = np.zeros((8, 128), np.float32)
    for g in (1, 2, 3):
        twiddle[2 * g - 2] = np.cos(2.0 * np.pi * g * e / WINDOW)
        twiddle[2 * g - 1] = np.sin(2.0 * np.pi * g * e / WINDOW)
    return high, low, twiddle


def reverse_bits(value, count):
    result = 0
    for bit in range(count):
        result = result + (value // 2**bit) % 2 * 2 ** (count - 1 - bit)
    return result


def scale_factor(sums_row):
    mean_square = jnp.sum(sums_row, axis=1, keepdims=True) / TOTAL
    return mean_square, lax.rsqrt(mean_square + 1e-06)


def exchange_kernel(
    x_hbm, high_hbm, low_hbm, twiddle_hbm, placed_ref, odd_ref, sums_ref,
    a_ref, high_ref, low_ref, twiddle_ref, bh_ref, bl_ref,
    send_ref, mid_a_ref, mid_b_ref, even_ref, zsum_ref, psum_ref,
    load_sem, table_sem, send_sem, recv_sem,
):
    outer, inner = lax.axis_index("outer"), lax.axis_index("inner")
    y, c, x, z = outer // 2, outer % 2, inner // 8, inner % 8
    plane = outer * 4 + x
    z_slot, p_slot = reverse_bits(z, 3), reverse_bits(plane, 5)
    z_index = z % 2 * 4 + z // 2
    slot = z_slot * 32 + p_slot

    def z_peer(there):
        return (outer, x * 8 + there)

    def plane_peer(t):
        dx, dc, dy = t % 4, t // 4 % 2, t // 8
        there_outer, there_x = (y + dy) % 4 * 2 + (c + dc) % 2, (x + dx) % 4
        return (there_outer, there_x * 8 + z), there_outer * 4 + there_x

    loads = []
    for number, (source, target) in enumerate((
        (high_hbm, high_ref), (low_hbm, low_ref), (twiddle_hbm, twiddle_ref),
    )):
        loads.append(pltpu.make_async_copy(source, target, table_sem.at[number]))
    for top in range(8):
        loads.append(
            pltpu.make_async_copy(
                x_hbm.at[pl.ds(512 * top, 512)],
                a_ref.at[pl.ds(PITCH * reverse_bits(top, 3), 512)],
                load_sem.at[top],
            )
        )
    for load in loads:
        load.start()

    barrier = pltpu.get_barrier_semaphore()
    for d in range(1, 8):
        pl.semaphore_signal(barrier, inc=1, device_id=z_peer((z + d) % 8), device_id_type=MESH)

    def greet(t, _):
        pl.semaphore_signal(barrier, inc=1, device_id=plane_peer(t)[0], device_id_type=MESH)
        return 0

    lax.fori_loop(1, 32, greet, 0)

    for load in loads:
        load.wait()

    twiddles = [
        (twiddle_ref[pl.ds(2 * g - 2, 1), :], twiddle_ref[pl.ds(2 * g - 1, 1), :]) for g in (1, 2, 3)
    ]
    step = 2.0 * math.pi * 2048 / TOTAL
    cos_step, sin_step = math.cos(step), math.sin(step)

    def spread(turn, carry):
        squares, phase_real, phase_imag = carry
        h = 31 - turn
        row = reverse_bits(h, 5)
        parts = [
            [a_ref[pl.ds((row + 32 * b) * 8 + q, 8, stride=PITCH), :] for q in range(8)] for b in range(2)
        ]
        for b in (1, 0):
            phase_real, phase_imag = (
                phase_real * cos_step + phase_imag * sin_step + parts[b][0],
                phase_imag * cos_step - phase_real * sin_step + parts[b][1],
            )
            for q in range(8):
                squares = squares + parts[b][q] * parts[b][q]
        v = [jnp.concatenate([parts[0][q], parts[1][q]], 0) for q in range(8)]
        real, imag = v[0::2], v[1::2]
        s02r, s02i = real[0] + real[2], imag[0] + imag[2]
        d02r, d02i = real[0] - real[2], imag[0] - imag[2]
        s13r, s13i = real[1] + real[3], imag[1] + imag[3]
        d13r, d13i = real[1] - real[3], imag[1] - imag[3]
        u = [
            (s02r + s13r, s02i + s13i),
            (d02r - d13i, d02i + d13r),
            (s02r - s13r, s02i - s13i),
            (d02r + d13i, d02i - d13r),
        ]
        rows = pl.ds(pl.multiple_of(h * 16, 16), 16)
        for g in range(4):
            ur, ui = u[g]
            if g:
                cosine, sine = twiddles[g - 1]
                ur, ui = ur * cosine - ui * sine, ur * sine + ui * cosine
            for s, value in ((0, ur), (1, ui)):
                high = value.astype(jnp.bfloat16)
                low = (value - high.astype(jnp.float32)).astype(jnp.bfloat16)
                bh_ref[g, rows, 128 * s : 128 * s + 128] = high
                bl_ref[g, rows, 128 * s : 128 * s + 128] = low
        return squares, phase_real, phase_imag

    zero = jnp.zeros((8, 128), jnp.float32)
    squares, phase_real, phase_imag = lax.fori_loop(0, 32, spread, (zero, zero, zero))

    lane = lax.broadcasted_iota(jnp.int32, (8, 128), 1)
    sub = lax.broadcasted_iota(jnp.int32, (8, 128), 0)
    angle = (sub * 256 + slot).astype(jnp.float32) * (2.0 * math.pi / TOTAL)
    cosine, sine = jnp.cos(angle), jnp.sin(angle)
    turned_real = jnp.where(lane == 1, phase_real * cosine + phase_imag * sine, 0.0)
    turned_imag = jnp.where(lane == 1, phase_imag * cosine - phase_real * sine, 0.0)
    mine = jnp.where(
        sub == 0,
        jnp.sum(squares, 0, keepdims=True),
        jnp.where(
            sub == 1,
            jnp.sum(turned_real, 0, keepdims=True),
            jnp.where(sub == 2, jnp.sum(turned_imag, 0, keepdims=True), 0.0),
        ),
    )
    zsum_ref[z] = mine

    def transform(g):
        def body(part, _):
            rows = pl.ds(pl.multiple_of(part * 256, 256), 256)
            bh, bl = bh_ref[g, rows, :], bl_ref[g, rows, :]
            dims = (((1,), (1,)), ((), ()))
            out = (
                lax.dot_general(high_ref[...], bh, dims, preferred_element_type=jnp.float32)
                + lax.dot_general(high_ref[...], bl, dims, preferred_element_type=jnp.float32)
                + lax.dot_general(low_ref[...], bh, dims, preferred_element_type=jnp.float32)
            )
            for s in range(2):
                for k in range(2):
                    first = g // 2 * 1024 + (part * 2 + k) * 2 + s
                    send_ref[g % 2, pl.ds(first, 128, stride=8), :] = out[
                        128 * s : 128 * s + 128, 128 * k : 128 * k + 128
                    ]
            return 0

        lax.fori_loop(0, 2, body, 0)

    def copy(peer, source, target, number):
        return pltpu.make_async_remote_copy(
            src_ref=source,
            dst_ref=target,
            send_sem=send_sem.at[number],
            recv_sem=recv_sem.at[number],
            device_id=peer,
            device_id_type=MESH,
        )

    def finish_recv(ref, number):
        copy(z_peer((z + 1) % 8), ref, ref, number).wait_recv()

    def finish_send(ref, number):
        copy(z_peer((z + 1) % 8), ref, ref, number).wait_send()

    even_send = send_ref.reshape(2, 8, 32, 8, 128).at[0]
    odd_send = send_ref.reshape(2, 8, 32, 8, 128).at[1]

    transform(0)
    pl.semaphore_wait(barrier, 38)
    for d in range(1, 8):
        copy(z_peer((z + d) % 8), zsum_ref.at[z], zsum_ref.at[z], 0).start()
    for parity in range(2):
        if parity:
            transform(2)
        for high_part in range(4):
            there = 2 * high_part + parity

            @pl.when(there != z)
            def _():
                copy(z_peer(there), even_send.at[4 * parity + high_part], mid_a_ref.at[z_slot], 1).start()

    transform(1)
    transform(3)

    def plane_bulk(source, target, number):
        def body(t, _):
            peer, there = plane_peer(t)
            copy(peer, source.at[:, there], target.at[:, p_slot], number).start()
            return 0

        lax.fori_loop(1, 32, body, 0)

    plane_bulk(odd_send, mid_b_ref, 2)
    mid_a_ref[z_slot] = even_send[z_index]
    for i in range(8):
        mid_b_ref[i, p_slot] = odd_send[i, plane]

    finish_recv(zsum_ref.at[pl.ds(0, 7)], 0)
    total = zsum_ref[0]
    for i in range(1, 8):
        total = total + zsum_ref[i]
    psum_ref[plane] = total

    def plane_sums(t, _):
        copy(plane_peer(t)[0], psum_ref.at[plane], psum_ref.at[plane], 3).start()
        return 0

    lax.fori_loop(1, 32, plane_sums, 0)

    finish_recv(mid_b_ref.at[:, pl.ds(0, 31)], 2)
    for d in (4, 3, 5, 2, 6, 1, 7):
        there = (z + d) % 8
        copy(z_peer(there), mid_b_ref.at[there % 2 * 4 + there // 2], odd_ref.at[z_slot], 4).start()
    odd_ref[z_slot] = mid_b_ref[z_index]

    finish_recv(psum_ref.at[pl.ds(0, 31)], 3)
    total = psum_ref[0]
    for i in range(1, 32):
        total = total + psum_ref[i]
    sums_ref[...] = total
    factor = scale_factor(total[0:1])[1]

    finish_recv(mid_a_ref.at[pl.ds(0, 7)], 1)
    plane_bulk(mid_a_ref, even_ref, 5)
    for i in range(8):
        even_ref[i, p_slot] = mid_a_ref[i, plane]
    finish_recv(even_ref.at[:, pl.ds(0, 31)], 5)
    even_rows = even_ref.reshape(2048, 128)

    def place(part, _):
        for s in range(2):
            for d in range(2):
                block = even_rows[pl.ds(d * 1024 + part * 2 + s, 128, stride=8), :]
                placed_ref[pl.ds(part * 512 + d * 2 + s, 128, stride=4), :] = block.T * factor
        return 0

    lax.fori_loop(0, 4, place, 0)

    finish_recv(odd_ref.at[pl.ds(0, 7)], 4)
    finish_send(zsum_ref.at[pl.ds(0, 7)], 0)
    finish_send(mid_a_ref.at[pl.ds(0, 7)], 1)
    finish_send(mid_b_ref.at[:, pl.ds(0, 31)], 2)
    finish_send(psum_ref.at[pl.ds(0, 31)], 3)
    finish_send(mid_b_ref.at[pl.ds(0, 7)], 4)
    finish_send(even_ref.at[:, pl.ds(0, 31)], 5)


def place_kernel(placed_ref, odd_ref, sums_ref, out_hbm, checks_ref, buffer_ref, sems):
    copies = [pltpu.make_async_copy(placed_ref, out_hbm.at[pl.ds(0, 2048)], sems.at[4])]
    copies[0].start()
    mean_square, factor = scale_factor(sums_ref[pl.ds(0, 1), :])
    for part in range(4):
        for s in range(2):
            for d in range(2):
                block = odd_ref[pl.ds(d * 1024 + part * 2 + s, 128, stride=8), :]
                buffer_ref[pl.ds(part * 512 + d * 2 + s, 128, stride=4), :] = block.T * factor
        copies.append(
            pltpu.make_async_copy(
                buffer_ref.at[pl.ds(part * 512, 512)],
                out_hbm.at[pl.ds(2048 + part * 512, 512)],
                sems.at[part],
            )
        )
        copies[-1].start()
    scale = factor * (math.sqrt(WINDOW) / math.sqrt(TOTAL))
    checks_ref[0] = mean_square[0, 0]
    for i in (1, 2):
        value = jnp.sum(sums_ref[pl.ds(i, 1), :], axis=1, keepdims=True) * scale
        checks_ref[i] = value[0, 0]
    for moved in copies:
        moved.wait()


def per_device(amplitudes):
    high, low, twiddle = dft_tables()
    rows = amplitudes.reshape(2, 2048, 128).transpose(1, 0, 2).reshape(4096, 128)
    vmem = pl.BlockSpec(memory_space=pltpu.VMEM)
    hbm = pl.BlockSpec(memory_space=pltpu.HBM)
    f32, bf16 = jnp.float32, jnp.bfloat16
    placed, odd, sums = pl.pallas_call(
        exchange_kernel,
        out_shape=(
            jax.ShapeDtypeStruct((2048, 128), f32),
            jax.ShapeDtypeStruct((8, 32, 8, 128), f32),
            jax.ShapeDtypeStruct((8, 128), f32),
        ),
        in_specs=[hbm, hbm, hbm, hbm],
        out_specs=(vmem, vmem, vmem),
        scratch_shapes=[
            pltpu.VMEM((8 * PITCH, 128), f32),
            pltpu.VMEM((256, 256), bf16),
            pltpu.VMEM((256, 256), bf16),
            pltpu.VMEM((8, 128), f32),
            pltpu.VMEM((4, 512, 256), bf16),
            pltpu.VMEM((4, 512, 256), bf16),
            pltpu.VMEM((2, 2048, 128), f32),
            pltpu.VMEM((8, 32, 8, 128), f32),
            pltpu.VMEM((8, 32, 8, 128), f32),
            pltpu.VMEM((8, 32, 8, 128), f32),
            pltpu.VMEM((8, 8, 128), f32),
            pltpu.VMEM((32, 8, 128), f32),
            pltpu.SemaphoreType.DMA((8,)),
            pltpu.SemaphoreType.DMA((3,)),
            pltpu.SemaphoreType.DMA((6,)),
            pltpu.SemaphoreType.DMA((6,)),
        ],
        compiler_params=pltpu.CompilerParams(
            collective_id=1, has_side_effects=True, vmem_limit_bytes=24 * 1024 * 1024
        ),
    )(rows, jnp.asarray(high), jnp.asarray(low), jnp.asarray(twiddle))
    out, checks = pl.pallas_call(
        place_kernel,
        out_shape=(
            jax.ShapeDtypeStruct((4096, 128), f32),
            jax.ShapeDtypeStruct((3,), f32),
        ),
        in_specs=[vmem, vmem, vmem],
        out_specs=(hbm, pl.BlockSpec(memory_space=pltpu.SMEM)),
        scratch_shapes=[pltpu.VMEM((2048, 128), f32), pltpu.SemaphoreType.DMA((5,))],
        compiler_params=pltpu.CompilerParams(vmem_limit_bytes=16 * 1024 * 1024),
    )(placed, odd.reshape(2048, 128), sums)
    transformed = out.reshape(2048, 2, 128).transpose(1, 0, 2).reshape(2, AMP_DEV)
    return transformed, checks


def solution(mesh):
    return jax.shard_map(
        per_device,
        mesh=mesh,
        in_specs=(P(None, AXES),),
        out_specs=(P(None, AXES), P()),
        check_vma=False,
    )
```

```python
import math

import jax
import jax.numpy as jnp
from jax import lax
from jax.experimental import pallas as pl
from jax.experimental.pallas import tpu as pltpu
from jax.sharding import PartitionSpec as P

MESH = pl.DeviceIdType.MESH
AXES = ("outer", "inner")
AMP_DEV = 262144
DEVICES = 256
TOTAL = AMP_DEV * DEVICES
WINDOW = 512
PITCH = 264
SPAN = 8 * PITCH


def reverse_bits(value, count):
    result = 0
    for bit in range(count):
        result = result + (value // 2**bit) % 2 * 2 ** (count - 1 - bit)
    return result


def scale_factor(sums_row):
    mean_square = jnp.sum(sums_row, axis=1, keepdims=True) / TOTAL
    return mean_square, lax.rsqrt(mean_square + 1e-06)


def exchange_kernel(
    x_hbm, placed_ref, late_ref, sums_ref,
    a_ref, high_ref, low_ref, bh_ref, bl_ref,
    send_ref, mid_a_ref, mid_b_ref, early_ref, zsum_ref, psum_ref,
    load_sem, send_sem, recv_sem,
):
    outer, inner = lax.axis_index("outer"), lax.axis_index("inner")
    y, c, x, z = outer // 2, outer % 2, inner // 8, inner % 8
    plane = outer * 4 + x
    z_slot, p_slot = reverse_bits(z, 3), reverse_bits(plane, 5)
    z_index = z % 2 * 4 + z // 2
    slot = z_slot * 32 + p_slot

    def z_peer(there):
        return (outer, x * 8 + there)

    def plane_peer(t):
        dx, dc, dy = t % 4, t // 4 % 2, t // 8
        there_outer, there_x = (y + dy) % 4 * 2 + (c + dc) % 2, (x + dx) % 4
        return (there_outer, there_x * 8 + z), there_outer * 4 + there_x

    loads = [
        [
            pltpu.make_async_copy(
                x_hbm.at[pl.ds(32 * top, 32), half],
                a_ref.at[half, reverse_bits(top, 3), pl.ds(0, 32)],
                load_sem.at[half, top],
            )
            for top in range(8)
        ]
        for half in range(2)
    ]
    for load in loads[0] + loads[1]:
        load.start()

    barrier = pltpu.get_barrier_semaphore()
    for d in range(1, 8):
        pl.semaphore_signal(barrier, inc=1, device_id=z_peer((z + d) % 8), device_id_type=MESH)

    def greet(t, _):
        pl.semaphore_signal(barrier, inc=1, device_id=plane_peer(t)[0], device_id_type=MESH)
        return 0

    lax.fori_loop(1, 32, greet, 0)

    lane = lax.broadcasted_iota(jnp.int32, (128, 128), 1)
    row = lax.broadcasted_iota(jnp.int32, (128, 128), 0)
    frequency = (row & 31) * 4 + (row >> 5)
    angle = ((frequency * lane) & 127).astype(jnp.float32) * (2.0 * math.pi / 128)
    for value, places in (
        (jnp.cos(angle) * WINDOW**-0.5, ((0, 0, 1.0), (1, 1, 1.0))),
        (jnp.sin(angle) * WINDOW**-0.5, ((1, 0, 1.0), (0, 1, -1.0))),
    ):
        high = value.astype(jnp.bfloat16)
        low = (value - high.astype(jnp.float32)).astype(jnp.bfloat16)
        for i, j, sign in places:
            high_ref[128 * i : 128 * i + 128, 128 * j : 128 * j + 128] = high * jnp.bfloat16(sign)
            low_ref[128 * i : 128 * i + 128, 128 * j : 128 * j + 128] = low * jnp.bfloat16(sign)
    lane = lax.broadcasted_iota(jnp.int32, (16, 128), 1)
    twiddles = []
    for g in (1, 2, 3):
        angle = (lane * g).astype(jnp.float32) * (2.0 * math.pi / WINDOW)
        twiddles.append((jnp.cos(angle), jnp.sin(angle)))

    step = 2.0 * math.pi * 2048 / TOTAL
    cos_step, sin_step = math.cos(step), math.sin(step)
    a_rows = a_ref.reshape(2 * SPAN, 128)
    zero = jnp.zeros((8, 128), jnp.float32)

    def spread_half(half, squares):
        for load in loads[half]:
            load.wait()

        def spread(turn, carry):
            squares, phase_real, phase_imag = carry
            h = 15 - turn
            middle = reverse_bits(h, 4)
            parts = [
                [
                    a_rows[pl.ds(half * SPAN + (middle + 16 * b) * 8 + q, 8, stride=PITCH), :]
                    for q in range(8)
                ]
                for b in range(2)
            ]
            for b in (1, 0):
                phase_real, phase_imag = (
                    phase_real * cos_step + phase_imag * sin_step + parts[b][0],
                    phase_imag * cos_step - phase_real * sin_step + parts[b][1],
                )
                for q in range(8):
                    squares = squares + parts[b][q] * parts[b][q]
            v = [jnp.concatenate([parts[0][q], parts[1][q]], 0) for q in range(8)]
            real, imag = v[0::2], v[1::2]
            s02r, s02i = real[0] + real[2], imag[0] + imag[2]
            d02r, d02i = real[0] - real[2], imag[0] - imag[2]
            s13r, s13i = real[1] + real[3], imag[1] + imag[3]
            d13r, d13i = real[1] - real[3], imag[1] - imag[3]
            u = [
                (s02r + s13r, s02i + s13i),
                (d02r - d13i, d02i + d13r),
                (s02r - s13r, s02i - s13i),
                (d02r + d13i, d02i - d13r),
            ]
            rows = pl.ds(pl.multiple_of(h * 16, 16), 16)
            for g in range(4):
                ur, ui = u[g]
                if g:
                    cosine, sine = twiddles[g - 1]
                    ur, ui = ur * cosine - ui * sine, ur * sine + ui * cosine
                for s, value in ((0, ur), (1, ui)):
                    high = value.astype(jnp.bfloat16)
                    low = (value - high.astype(jnp.float32)).astype(jnp.bfloat16)
                    bh_ref[g, rows, 128 * s : 128 * s + 128] = high
                    bl_ref[g, rows, 128 * s : 128 * s + 128] = low
            return squares, phase_real, phase_imag

        return lax.fori_loop(0, 16, spread, (squares, zero, zero))

    def transform(half, first):
        def body(f, _):
            g = first + f
            bh, bl = bh_ref[g], bl_ref[g]
            dims = (((1,), (1,)), ((), ()))
            out = (
                lax.dot_general(high_ref[...], bh, dims, preferred_element_type=jnp.float32)
                + lax.dot_general(high_ref[...], bl, dims, preferred_element_type=jnp.float32)
                + lax.dot_general(low_ref[...], bh, dims, preferred_element_type=jnp.float32)
            )
            for k in range(2):
                for s in range(2):
                    place = pl.ds(first // 2 * 1024 + f * 4 + k * 2 + s, 128, stride=8)
                    send_ref[half, place, :] = out[128 * s : 128 * s + 128, 128 * k : 128 * k + 128]
            return 0

        lax.fori_loop(0, 2, body, 0)

    def copy(peer, source, target, number):
        return pltpu.make_async_remote_copy(
            src_ref=source,
            dst_ref=target,
            send_sem=send_sem.at[number],
            recv_sem=recv_sem.at[number],
            device_id=peer,
            device_id_type=MESH,
        )

    def finish_recv(ref, number):
        copy(z_peer((z + 1) % 8), ref, ref, number).wait_recv()

    def finish_send(ref, number):
        copy(z_peer((z + 1) % 8), ref, ref, number).wait_send()

    early_send = send_ref.reshape(2, 8, 32, 8, 128).at[0]
    late_send = send_ref.reshape(2, 8, 32, 8, 128).at[1]

    squares, phase_real_0, phase_imag_0 = spread_half(0, zero)
    transform(0, 0)
    pl.semaphore_wait(barrier, 38)
    for parity in range(2):
        if parity:
            transform(0, 2)
        for high_part in range(4):
            there = 2 * high_part + parity

            @pl.when(there != z)
            def _():
                copy(z_peer(there), early_send.at[4 * parity + high_part], mid_a_ref.at[z_slot], 1).start()

    squares, phase_real_1, phase_imag_1 = spread_half(1, squares)
    transform(1, 0)
    transform(1, 2)

    def plane_bulk(source, target, number):
        def body(t, _):
            peer, there = plane_peer(t)
            copy(peer, source.at[:, there], target.at[:, p_slot], number).start()
            return 0

        lax.fori_loop(1, 32, body, 0)

    plane_bulk(late_send, mid_b_ref, 2)
    mid_a_ref[z_slot] = early_send[z_index]
    for i in range(8):
        mid_b_ref[i, p_slot] = late_send[i, plane]

    lane = lax.broadcasted_iota(jnp.int32, (8, 128), 1)
    sub = lax.broadcasted_iota(jnp.int32, (8, 128), 0)
    turned_real, turned_imag = zero, zero
    for half, phase_real, phase_imag in ((0, phase_real_0, phase_imag_0), (1, phase_real_1, phase_imag_1)):
        angle = (half * 65536 + sub * 256 + slot).astype(jnp.float32) * (2.0 * math.pi / TOTAL)
        cosine, sine = jnp.cos(angle), jnp.sin(angle)
        turned_real = turned_real + (phase_real * cosine + phase_imag * sine)
        turned_imag = turned_imag + (phase_imag * cosine - phase_real * sine)
    turned_real = jnp.where(lane == 1, turned_real, 0.0)
    turned_imag = jnp.where(lane == 1, turned_imag, 0.0)
    zsum_ref[z] = jnp.where(
        sub == 0,
        jnp.sum(squares, 0, keepdims=True),
        jnp.where(
            sub == 1,
            jnp.sum(turned_real, 0, keepdims=True),
            jnp.where(sub == 2, jnp.sum(turned_imag, 0, keepdims=True), 0.0),
        ),
    )
    for d in range(1, 8):
        copy(z_peer((z + d) % 8), zsum_ref.at[z], zsum_ref.at[z], 0).start()

    finish_recv(mid_b_ref.at[:, pl.ds(0, 31)], 2)
    for d in (4, 3, 5, 2, 6, 1, 7):
        there = (z + d) % 8
        copy(z_peer(there), mid_b_ref.at[there % 2 * 4 + there // 2], late_ref.at[z_slot], 4).start()
    late_ref[z_slot] = mid_b_ref[z_index]

    finish_recv(zsum_ref.at[pl.ds(0, 7)], 0)
    total = zsum_ref[0]
    for i in range(1, 8):
        total = total + zsum_ref[i]
    psum_ref[plane] = total

    def plane_sums(t, _):
        copy(plane_peer(t)[0], psum_ref.at[plane], psum_ref.at[plane], 3).start()
        return 0

    lax.fori_loop(1, 32, plane_sums, 0)

    finish_recv(mid_a_ref.at[pl.ds(0, 7)], 1)
    plane_bulk(mid_a_ref, early_ref, 5)
    for i in range(8):
        early_ref[i, p_slot] = mid_a_ref[i, plane]

    finish_recv(psum_ref.at[pl.ds(0, 31)], 3)
    total = psum_ref[0]
    for i in range(1, 32):
        total = total + psum_ref[i]
    sums_ref[...] = total
    factor = scale_factor(total[0:1])[1]

    finish_recv(early_ref.at[:, pl.ds(0, 31)], 5)
    place_rows(early_ref.reshape(2048, 128), placed_ref, factor)

    finish_recv(late_ref.at[pl.ds(0, 7)], 4)
    finish_send(zsum_ref.at[pl.ds(0, 7)], 0)
    finish_send(mid_a_ref.at[pl.ds(0, 7)], 1)
    finish_send(mid_b_ref.at[:, pl.ds(0, 31)], 2)
    finish_send(psum_ref.at[pl.ds(0, 31)], 3)
    finish_send(mid_b_ref.at[pl.ds(0, 7)], 4)
    finish_send(early_ref.at[:, pl.ds(0, 31)], 5)


def place_rows(source, target, factor):
    def body(part, _):
        place_part(source, target, factor, part)
        return 0

    lax.fori_loop(0, 4, body, 0)


def place_part(source, target, factor, part):
    for s in range(2):
        for d in range(2):
            block = source[pl.ds(d * 1024 + part * 2 + s, 128, stride=8), :]
            target[pl.ds(part * 512 + d * 2 + s, 128, stride=4), :] = block.T * factor


def place_kernel(placed_ref, late_ref, sums_ref, out_hbm, checks_ref, buffer_ref, sems):
    copies = []

    def move(source, first, size, number):
        copies.append(pltpu.make_async_copy(source, out_hbm.at[pl.ds(first, size)], sems.at[number]))
        copies[-1].start()

    for f in range(2):
        move(placed_ref.at[pl.ds(f * 1024, 1024)], f * 2048, 1024, f)
    mean_square, factor = scale_factor(sums_ref[pl.ds(0, 1), :])
    for part in range(4):
        place_part(late_ref, buffer_ref, factor, part)
        first = part // 2 * 2048 + 1024 + part % 2 * 512
        move(buffer_ref.at[pl.ds(part * 512, 512)], first, 512, 2 + part)
    scale = factor * (math.sqrt(WINDOW) / math.sqrt(TOTAL))
    checks_ref[0] = mean_square[0, 0]
    for i in (1, 2):
        value = jnp.sum(sums_ref[pl.ds(i, 1), :], axis=1, keepdims=True) * scale
        checks_ref[i] = value[0, 0]
    for moved in copies:
        moved.wait()


def per_device(amplitudes):
    rows = amplitudes.reshape(2, 2048, 128).transpose(1, 0, 2).reshape(256, 2, 8, 128)
    vmem = pl.BlockSpec(memory_space=pltpu.VMEM)
    hbm = pl.BlockSpec(memory_space=pltpu.HBM)
    f32, bf16 = jnp.float32, jnp.bfloat16
    placed, late, sums = pl.pallas_call(
        exchange_kernel,
        out_shape=(
            jax.ShapeDtypeStruct((2048, 128), f32),
            jax.ShapeDtypeStruct((8, 32, 8, 128), f32),
            jax.ShapeDtypeStruct((8, 128), f32),
        ),
        in_specs=[hbm],
        out_specs=(vmem, vmem, vmem),
        scratch_shapes=[
            pltpu.VMEM((2, 8, 33, 8, 128), f32),
            pltpu.VMEM((256, 256), bf16),
            pltpu.VMEM((256, 256), bf16),
            pltpu.VMEM((4, 256, 256), bf16),
            pltpu.VMEM((4, 256, 256), bf16),
            pltpu.VMEM((2, 2048, 128), f32),
            pltpu.VMEM((8, 32, 8, 128), f32),
            pltpu.VMEM((8, 32, 8, 128), f32),
            pltpu.VMEM((8, 32, 8, 128), f32),
            pltpu.VMEM((8, 8, 128), f32),
            pltpu.VMEM((32, 8, 128), f32),
            pltpu.SemaphoreType.DMA((2, 8)),
            pltpu.SemaphoreType.DMA((6,)),
            pltpu.SemaphoreType.DMA((6,)),
        ],
        compiler_params=pltpu.CompilerParams(
            collective_id=1, has_side_effects=True, vmem_limit_bytes=51 * 1024 * 1024
        ),
    )(rows)
    out, checks = pl.pallas_call(
        place_kernel,
        out_shape=(
            jax.ShapeDtypeStruct((4096, 128), f32),
            jax.ShapeDtypeStruct((3,), f32),
        ),
        in_specs=[vmem, vmem, vmem],
        out_specs=(hbm, pl.BlockSpec(memory_space=pltpu.SMEM)),
        scratch_shapes=[pltpu.VMEM((2048, 128), f32), pltpu.SemaphoreType.DMA((6,))],
        compiler_params=pltpu.CompilerParams(vmem_limit_bytes=16 * 1024 * 1024),
    )(placed, late.reshape(2048, 128), sums)
    transformed = out.reshape(2048, 2, 128).transpose(1, 0, 2).reshape(2, AMP_DEV)
    return transformed, checks


def solution(mesh):
    return jax.shard_map(
        per_device,
        mesh=mesh,
        in_specs=(P(None, AXES),),
        out_specs=(P(None, AXES), P()),
        check_vma=False,
    )
```

```python
import math

import jax
import jax.numpy as jnp
from jax import lax
from jax.experimental import pallas as pl
from jax.experimental.pallas import tpu as pltpu
from jax.sharding import PartitionSpec as P

MESH = pl.DeviceIdType.MESH
AXES = ("outer", "inner")
AMP_DEV = 262144
DEVICES = 256
TOTAL = AMP_DEV * DEVICES
WINDOW = 512
PITCH = 264
SPAN = 8 * PITCH


def reverse_bits(value, count):
    result = 0
    for bit in range(count):
        result = result + (value // 2**bit) % 2 * 2 ** (count - 1 - bit)
    return result


def scale_factor(squares):
    mean_square = squares / TOTAL
    return mean_square, lax.rsqrt(mean_square + 1e-06)


def exchange_kernel(
    x_hbm, placed_ref, late_ref, sums_ref,
    a_ref, high_ref, low_ref, bh_ref, bl_ref,
    send_ref, mid_a_ref, mid_b_ref, early_ref, zsum_ref, psum_ref,
    load_sem, send_sem, recv_sem, round_sem,
):
    outer, inner = lax.axis_index("outer"), lax.axis_index("inner")
    y, c, x, z = outer // 2, outer % 2, inner // 8, inner % 8
    plane = outer * 4 + x
    z_slot, p_slot = reverse_bits(z, 3), reverse_bits(plane, 5)
    z_index = z % 2 * 4 + z // 2
    slot = z_slot * 32 + p_slot

    def z_peer(there):
        return (outer, x * 8 + there)

    def plane_peer(t):
        dx, dy, dc = t % 4, (t % 4 + t // 4) % 4, (t + t // 16) % 2
        there_outer, there_x = (y + dy) % 4 * 2 + (c + dc) % 2, (x + dx) % 4
        return (there_outer, there_x * 8 + z), there_outer * 4 + there_x

    loads = [
        [
            pltpu.make_async_copy(
                x_hbm.at[pl.ds(32 * top, 32), half],
                a_ref.at[half, reverse_bits(top, 3), pl.ds(0, 32)],
                load_sem.at[half, top],
            )
            for top in range(8)
        ]
        for half in range(2)
    ]
    for load in loads[0] + loads[1]:
        load.start()

    barrier = pltpu.get_barrier_semaphore()
    for d in range(1, 8):
        pl.semaphore_signal(barrier, inc=1, device_id=z_peer((z + d) % 8), device_id_type=MESH)

    def greet(t, _):
        pl.semaphore_signal(barrier, inc=1, device_id=plane_peer(t)[0], device_id_type=MESH)
        return 0

    @pl.when(z == 0)
    def _():
        lax.fori_loop(1, 32, greet, 0)

    lane = lax.broadcasted_iota(jnp.int32, (128, 128), 1)
    row = lax.broadcasted_iota(jnp.int32, (128, 128), 0)
    frequency = (row & 31) * 4 + (row >> 5)
    angle = ((frequency * lane) & 127).astype(jnp.float32) * (2.0 * math.pi / 128)
    for value, places in (
        (jnp.cos(angle) * WINDOW**-0.5, ((0, 0, 1.0), (1, 1, 1.0))),
        (jnp.sin(angle) * WINDOW**-0.5, ((1, 0, 1.0), (0, 1, -1.0))),
    ):
        high = value.astype(jnp.bfloat16)
        low = (value - high.astype(jnp.float32)).astype(jnp.bfloat16)
        for i, j, sign in places:
            high_ref[128 * i : 128 * i + 128, 128 * j : 128 * j + 128] = high * jnp.bfloat16(sign)
            low_ref[128 * i : 128 * i + 128, 128 * j : 128 * j + 128] = low * jnp.bfloat16(sign)
    lane = lax.broadcasted_iota(jnp.int32, (16, 128), 1)
    twiddles = []
    for g in (1, 2, 3):
        angle = (lane * g).astype(jnp.float32) * (2.0 * math.pi / WINDOW)
        twiddles.append((jnp.cos(angle), jnp.sin(angle)))

    step = 2.0 * math.pi * 2048 / TOTAL
    cos_step, sin_step = math.cos(step), math.sin(step)
    a_rows = a_ref.reshape(2 * SPAN, 128)
    zero = jnp.zeros((8, 128), jnp.float32)

    def spread_half(half, squares):
        for load in loads[half]:
            load.wait()

        def spread(turn, carry):
            squares, phase_real, phase_imag = carry
            h = 15 - turn
            middle = reverse_bits(h, 4)
            parts = [
                [
                    a_rows[pl.ds(half * SPAN + (middle + 16 * b) * 8 + q, 8, stride=PITCH), :]
                    for q in range(8)
                ]
                for b in range(2)
            ]
            for b in (1, 0):
                phase_real, phase_imag = (
                    phase_real * cos_step + phase_imag * sin_step + parts[b][0],
                    phase_imag * cos_step - phase_real * sin_step + parts[b][1],
                )
                for q in range(8):
                    squares = squares + parts[b][q] * parts[b][q]
            v = [jnp.concatenate([parts[0][q], parts[1][q]], 0) for q in range(8)]
            real, imag = v[0::2], v[1::2]
            s02r, s02i = real[0] + real[2], imag[0] + imag[2]
            d02r, d02i = real[0] - real[2], imag[0] - imag[2]
            s13r, s13i = real[1] + real[3], imag[1] + imag[3]
            d13r, d13i = real[1] - real[3], imag[1] - imag[3]
            u = [
                (s02r + s13r, s02i + s13i),
                (d02r - d13i, d02i + d13r),
                (s02r - s13r, s02i - s13i),
                (d02r + d13i, d02i - d13r),
            ]
            rows = pl.ds(pl.multiple_of(h * 16, 16), 16)
            for g in range(4):
                ur, ui = u[g]
                if g:
                    cosine, sine = twiddles[g - 1]
                    ur, ui = ur * cosine - ui * sine, ur * sine + ui * cosine
                for s, value in ((0, ur), (1, ui)):
                    high = value.astype(jnp.bfloat16)
                    low = (value - high.astype(jnp.float32)).astype(jnp.bfloat16)
                    bh_ref[g, rows, 128 * s : 128 * s + 128] = high
                    bl_ref[g, rows, 128 * s : 128 * s + 128] = low
            return squares, phase_real, phase_imag

        return lax.fori_loop(0, 16, spread, (squares, zero, zero))

    def transform(half, first):
        def body(f, _):
            g = first + f
            bh, bl = bh_ref[g], bl_ref[g]
            dims = (((1,), (1,)), ((), ()))
            out = (
                lax.dot_general(high_ref[...], bh, dims, preferred_element_type=jnp.float32)
                + lax.dot_general(high_ref[...], bl, dims, preferred_element_type=jnp.float32)
                + lax.dot_general(low_ref[...], bh, dims, preferred_element_type=jnp.float32)
            )
            for k in range(2):
                for s in range(2):
                    place = pl.ds(first // 2 * 1024 + f * 4 + k * 2 + s, 128, stride=8)
                    send_ref[half, place, :] = out[128 * s : 128 * s + 128, 128 * k : 128 * k + 128]
            return 0

        lax.fori_loop(0, 2, body, 0)

    def copy(peer, source, target, number):
        return pltpu.make_async_remote_copy(
            src_ref=source,
            dst_ref=target,
            send_sem=send_sem.at[number],
            recv_sem=recv_sem.at[number],
            device_id=peer,
            device_id_type=MESH,
        )

    def finish_recv(ref, number):
        copy(z_peer((z + 1) % 8), ref, ref, number).wait_recv()

    def finish_send(ref, number):
        copy(z_peer((z + 1) % 8), ref, ref, number).wait_send()

    early_send = send_ref.reshape(2, 8, 32, 8, 128).at[0]
    late_send = send_ref.reshape(2, 8, 32, 8, 128).at[1]

    squares, phase_real_0, phase_imag_0 = spread_half(0, zero)
    transform(0, 0)
    transform(0, 2)
    pl.semaphore_wait(barrier, 7 + jnp.where(z == 0, 31, 0))

    def early_z(there):
        copy(z_peer(there), early_send.at[there % 2 * 4 + there // 2], mid_a_ref.at[z_slot], 1).start()

    for d in (4, 3, 5, 2, 6, 1, 7):
        early_z((z + d) % 8)

    def line_ready(t, _):
        pl.semaphore_signal(round_sem.at[0], inc=1, device_id=plane_peer(t)[0], device_id_type=MESH)
        return 0

    @pl.when(z == 0)
    def _():
        lax.fori_loop(1, 32, line_ready, 0)

    squares, phase_real_1, phase_imag_1 = spread_half(1, squares)
    transform(1, 0)
    transform(1, 2)

    @pl.when(z == 0)
    def _():
        pl.semaphore_wait(round_sem.at[0], 31)
        for there in range(1, 8):
            pl.semaphore_signal(round_sem.at[1], inc=1, device_id=z_peer(there), device_id_type=MESH)

    @pl.when(z != 0)
    def _():
        pl.semaphore_wait(round_sem.at[1], 1)

    def plane_bulk(source, target, number):
        def body(t, _):
            peer, there = plane_peer(t)
            copy(peer, source.at[:, there], target.at[:, p_slot], number).start()
            return 0

        lax.fori_loop(1, 32, body, 0)

    plane_bulk(late_send, mid_b_ref, 2)
    mid_a_ref[z_slot] = early_send[z_index]
    for i in range(8):
        mid_b_ref[i, p_slot] = late_send[i, plane]

    column = lax.broadcasted_iota(jnp.int32, (8, 128), 1)
    sub = lax.broadcasted_iota(jnp.int32, (8, 128), 0)
    turned_real, turned_imag = zero, zero
    for half, phase_real, phase_imag in ((0, phase_real_0, phase_imag_0), (1, phase_real_1, phase_imag_1)):
        angle = (half * 65536 + sub * 256 + slot).astype(jnp.float32) * (2.0 * math.pi / TOTAL)
        cosine, sine = jnp.cos(angle), jnp.sin(angle)
        turned_real = turned_real + (phase_real * cosine + phase_imag * sine)
        turned_imag = turned_imag + (phase_imag * cosine - phase_real * sine)
    lane = lax.broadcasted_iota(jnp.int32, (1, 128), 1)
    row = jnp.zeros((1, 128), jnp.float32)
    for i, value in enumerate((
        squares, jnp.where(column == 1, turned_real, 0.0), jnp.where(column == 1, turned_imag, 0.0),
    )):
        summed = jnp.sum(jnp.sum(value, 0, keepdims=True), 1, keepdims=True)
        row = jnp.where(lane == i, summed, row)
    zsum_ref[z] = row
    for d in range(1, 8):
        copy(z_peer((z + d) % 8), zsum_ref.at[z], zsum_ref.at[z], 0).start()

    finish_recv(mid_b_ref.at[:, pl.ds(0, 31)], 2)
    def late_z(there):
        copy(z_peer(there), mid_b_ref.at[there % 2 * 4 + there // 2], late_ref.at[z_slot], 4).start()

    for d in (4, 3, 5, 2, 6, 1, 7):
        late_z((z + d) % 8)

    late_ref[z_slot] = mid_b_ref[z_index]

    finish_recv(zsum_ref.at[pl.ds(0, 7)], 0)
    total = zsum_ref[0]
    for i in range(1, 8):
        total = total + zsum_ref[i]
    psum_ref[plane] = total

    def plane_sums(t, _):
        copy(plane_peer(t)[0], psum_ref.at[plane], psum_ref.at[plane], 3).start()
        return 0

    lax.fori_loop(1, 32, plane_sums, 0)

    finish_recv(mid_a_ref.at[pl.ds(0, 7)], 1)
    plane_bulk(mid_a_ref, early_ref, 5)
    for i in range(8):
        early_ref[i, p_slot] = mid_a_ref[i, plane]

    finish_recv(psum_ref.at[pl.ds(0, 31)], 3)
    total = psum_ref[0]
    for i in range(1, 32):
        total = total + psum_ref[i]
    sums_ref[...] = total
    factor = scale_factor(total[:, 0:1])[1]

    finish_recv(early_ref.at[:, pl.ds(0, 31)], 5)
    place_rows(early_ref.reshape(2048, 128), placed_ref, factor)

    finish_recv(late_ref.at[pl.ds(0, 7)], 4)
    finish_send(zsum_ref.at[pl.ds(0, 7)], 0)
    finish_send(mid_a_ref.at[pl.ds(0, 7)], 1)
    finish_send(mid_b_ref.at[:, pl.ds(0, 31)], 2)
    finish_send(psum_ref.at[pl.ds(0, 31)], 3)
    finish_send(mid_b_ref.at[pl.ds(0, 7)], 4)
    finish_send(early_ref.at[:, pl.ds(0, 31)], 5)


def place_rows(source, target, factor):
    def body(part, _):
        place_part(source, target, factor, part)
        return 0

    lax.fori_loop(0, 4, body, 0)


def place_part(source, target, factor, part):
    for s in range(2):
        for d in range(2):
            block = source[pl.ds(d * 1024 + part * 2 + s, 128, stride=8), :]
            target[pl.ds(part * 512 + d * 2 + s, 128, stride=4), :] = block.T * factor


def place_kernel(placed_ref, late_ref, sums_ref, out_hbm, checks_ref, buffer_ref, sems):
    copies = []

    def move(source, first, size, number):
        copies.append(pltpu.make_async_copy(source, out_hbm.at[pl.ds(first, size)], sems.at[number]))
        copies[-1].start()

    for f in range(2):
        move(placed_ref.at[pl.ds(f * 1024, 1024)], f * 2048, 1024, f)
    sums = sums_ref[...]
    mean_square, factor = scale_factor(sums[:, 0:1])
    for part in range(4):
        place_part(late_ref, buffer_ref, factor, part)
        first = part // 2 * 2048 + 1024 + part % 2 * 512
        move(buffer_ref.at[pl.ds(part * 512, 512)], first, 512, 2 + part)
    scale = factor * (math.sqrt(WINDOW) / math.sqrt(TOTAL))
    checks_ref[0] = mean_square[0, 0]
    for i in (1, 2):
        checks_ref[i] = (sums[:, i : i + 1] * scale)[0, 0]
    for moved in copies:
        moved.wait()


def per_device(amplitudes):
    rows = amplitudes.reshape(2, 2048, 128).transpose(1, 0, 2).reshape(256, 2, 8, 128)
    vmem = pl.BlockSpec(memory_space=pltpu.VMEM)
    hbm = pl.BlockSpec(memory_space=pltpu.HBM)
    f32, bf16 = jnp.float32, jnp.bfloat16
    placed, late, sums = pl.pallas_call(
        exchange_kernel,
        out_shape=(
            jax.ShapeDtypeStruct((2048, 128), f32),
            jax.ShapeDtypeStruct((8, 32, 8, 128), f32),
            jax.ShapeDtypeStruct((1, 128), f32),
        ),
        in_specs=[hbm],
        out_specs=(vmem, vmem, vmem),
        scratch_shapes=[
            pltpu.VMEM((2, 8, 33, 8, 128), f32),
            pltpu.VMEM((256, 256), bf16),
            pltpu.VMEM((256, 256), bf16),
            pltpu.VMEM((4, 256, 256), bf16),
            pltpu.VMEM((4, 256, 256), bf16),
            pltpu.VMEM((2, 2048, 128), f32),
            pltpu.VMEM((8, 32, 8, 128), f32),
            pltpu.VMEM((8, 32, 8, 128), f32),
            pltpu.VMEM((8, 32, 8, 128), f32),
            pltpu.VMEM((8, 1, 128), f32),
            pltpu.VMEM((32, 1, 128), f32),
            pltpu.SemaphoreType.DMA((2, 8)),
            pltpu.SemaphoreType.DMA((6,)),
            pltpu.SemaphoreType.DMA((6,)),
            pltpu.SemaphoreType.REGULAR((2,)),
        ],
        compiler_params=pltpu.CompilerParams(
            collective_id=1, has_side_effects=True, vmem_limit_bytes=51 * 1024 * 1024
        ),
    )(rows)
    out, checks = pl.pallas_call(
        place_kernel,
        out_shape=(
            jax.ShapeDtypeStruct((4096, 128), f32),
            jax.ShapeDtypeStruct((3,), f32),
        ),
        in_specs=[vmem, vmem, vmem],
        out_specs=(hbm, pl.BlockSpec(memory_space=pltpu.SMEM)),
        scratch_shapes=[pltpu.VMEM((2048, 128), f32), pltpu.SemaphoreType.DMA((6,))],
        compiler_params=pltpu.CompilerParams(vmem_limit_bytes=16 * 1024 * 1024),
    )(placed, late.reshape(2048, 128), sums)
    transformed = out.reshape(2048, 2, 128).transpose(1, 0, 2).reshape(2, AMP_DEV)
    return transformed, checks


def solution(mesh):
    return jax.shard_map(
        per_device,
        mesh=mesh,
        in_specs=(P(None, AXES),),
        out_specs=(P(None, AXES), P()),
        check_vma=False,
    )
```

```python
import math

import jax
import jax.numpy as jnp
from jax import lax
from jax.experimental import pallas as pl
from jax.experimental.pallas import tpu as pltpu
from jax.sharding import PartitionSpec as P

MESH = pl.DeviceIdType.MESH
AXES = ("outer", "inner")
AMP_DEV = 262144
DEVICES = 256
TOTAL = AMP_DEV * DEVICES
WINDOW = 512
PITCH = 264
SPAN = 8 * PITCH


def reverse_bits(value, count):
    result = 0
    for bit in range(count):
        result = result + (value // 2**bit) % 2 * 2 ** (count - 1 - bit)
    return result


def scale_factor(squares):
    mean_square = squares / TOTAL
    return mean_square, lax.rsqrt(mean_square + 1e-06)


def exchange_kernel(
    x_hbm, placed_ref, late_ref, sums_ref,
    a_ref, high_ref, low_ref, bh_ref, bl_ref,
    send_ref, mid_a_ref, mid_b_ref, early_ref, zsum_ref, psum_ref,
    load_sem, send_sem, recv_sem, round_sem,
):
    loads = [
        [
            pltpu.make_async_copy(
                x_hbm.at[pl.ds(32 * top, 32), half],
                a_ref.at[half, reverse_bits(top, 3), pl.ds(0, 32)],
                load_sem.at[half, top],
            )
            for top in range(8)
        ]
        for half in range(2)
    ]
    for load in loads[0]:
        load.start()

    outer, inner = lax.axis_index("outer"), lax.axis_index("inner")
    y, c, x, z = outer // 2, outer % 2, inner // 8, inner % 8
    plane = outer * 4 + x
    z_slot, p_slot = reverse_bits(z, 3), reverse_bits(plane, 5)
    z_index = z % 2 * 4 + z // 2
    slot = z_slot * 32 + p_slot

    def z_peer(there):
        return (outer, x * 8 + there)

    def plane_peer(t):
        dx, dy, dc = t % 4, (t % 4 + t // 4) % 4, (t + t // 16) % 2
        there_outer, there_x = (y + dy) % 4 * 2 + (c + dc) % 2, (x + dx) % 4
        return (there_outer, there_x * 8 + z), there_outer * 4 + there_x

    barrier = pltpu.get_barrier_semaphore()
    for d in range(1, 8):
        pl.semaphore_signal(barrier, inc=1, device_id=z_peer((z + d) % 8), device_id_type=MESH)

    def greet(t, _):
        pl.semaphore_signal(barrier, inc=1, device_id=plane_peer(t)[0], device_id_type=MESH)
        return 0

    @pl.when(z == 0)
    def _():
        lax.fori_loop(1, 32, greet, 0)

    lane = lax.broadcasted_iota(jnp.int32, (128, 128), 1)
    row = lax.broadcasted_iota(jnp.int32, (128, 128), 0)
    frequency = (row & 31) * 4 + (row >> 5)
    angle = ((frequency * lane) & 127).astype(jnp.float32) * (2.0 * math.pi / 128)
    for value, places in (
        (jnp.cos(angle) * WINDOW**-0.5, ((0, 0, 1.0), (1, 1, 1.0))),
        (jnp.sin(angle) * WINDOW**-0.5, ((1, 0, 1.0), (0, 1, -1.0))),
    ):
        high = value.astype(jnp.bfloat16)
        low = (value - high.astype(jnp.float32)).astype(jnp.bfloat16)
        for i, j, sign in places:
            high_ref[128 * i : 128 * i + 128, 128 * j : 128 * j + 128] = high * jnp.bfloat16(sign)
            low_ref[128 * i : 128 * i + 128, 128 * j : 128 * j + 128] = low * jnp.bfloat16(sign)
    lane = lax.broadcasted_iota(jnp.int32, (16, 128), 1)
    twiddles = []
    for g in (1, 2, 3):
        angle = (lane * g).astype(jnp.float32) * (2.0 * math.pi / WINDOW)
        twiddles.append((jnp.cos(angle), jnp.sin(angle)))

    step = 2.0 * math.pi * 2048 / TOTAL
    cos_step, sin_step = math.cos(step), math.sin(step)
    a_rows = a_ref.reshape(2 * SPAN, 128)
    zero = jnp.zeros((8, 128), jnp.float32)

    def spread_half(half, squares):
        for load in loads[half]:
            load.wait()
        if half == 0:
            for load in loads[1]:
                load.start()

        def spread(turn, carry):
            squares, phase_real, phase_imag = carry
            h = 15 - turn
            middle = reverse_bits(h, 4)
            parts = [
                [
                    a_rows[pl.ds(half * SPAN + (middle + 16 * b) * 8 + q, 8, stride=PITCH), :]
                    for q in range(8)
                ]
                for b in range(2)
            ]
            for b in (1, 0):
                phase_real, phase_imag = (
                    phase_real * cos_step + phase_imag * sin_step + parts[b][0],
                    phase_imag * cos_step - phase_real * sin_step + parts[b][1],
                )
                for q in range(8):
                    squares = squares + parts[b][q] * parts[b][q]
            v = [jnp.concatenate([parts[0][q], parts[1][q]], 0) for q in range(8)]
            real, imag = v[0::2], v[1::2]
            s02r, s02i = real[0] + real[2], imag[0] + imag[2]
            d02r, d02i = real[0] - real[2], imag[0] - imag[2]
            s13r, s13i = real[1] + real[3], imag[1] + imag[3]
            d13r, d13i = real[1] - real[3], imag[1] - imag[3]
            u = [
                (s02r + s13r, s02i + s13i),
                (d02r - d13i, d02i + d13r),
                (s02r - s13r, s02i - s13i),
                (d02r + d13i, d02i - d13r),
            ]
            rows = pl.ds(pl.multiple_of(h * 16, 16), 16)
            for g in range(4):
                ur, ui = u[g]
                if g:
                    cosine, sine = twiddles[g - 1]
                    ur, ui = ur * cosine - ui * sine, ur * sine + ui * cosine
                for s, value in ((0, ur), (1, ui)):
                    high = value.astype(jnp.bfloat16)
                    low = (value - high.astype(jnp.float32)).astype(jnp.bfloat16)
                    bh_ref[g, rows, 128 * s : 128 * s + 128] = high
                    bl_ref[g, rows, 128 * s : 128 * s + 128] = low
            return squares, phase_real, phase_imag

        return lax.fori_loop(0, 16, spread, (squares, zero, zero))

    def transform(half, first):
        for f in range(2):
            bh, bl = bh_ref[first + f], bl_ref[first + f]
            dims = (((1,), (1,)), ((), ()))
            out = (
                lax.dot_general(high_ref[...], bh, dims, preferred_element_type=jnp.float32)
                + lax.dot_general(high_ref[...], bl, dims, preferred_element_type=jnp.float32)
                + lax.dot_general(low_ref[...], bh, dims, preferred_element_type=jnp.float32)
            )
            for k in range(2):
                for s in range(2):
                    place = pl.ds(first // 2 * 1024 + f * 4 + k * 2 + s, 128, stride=8)
                    send_ref[half, place, :] = out[128 * s : 128 * s + 128, 128 * k : 128 * k + 128]

    def copy(peer, source, target, number):
        return pltpu.make_async_remote_copy(
            src_ref=source,
            dst_ref=target,
            send_sem=send_sem.at[number],
            recv_sem=recv_sem.at[number],
            device_id=peer,
            device_id_type=MESH,
        )

    def finish_recv(ref, number):
        copy(z_peer((z + 1) % 8), ref, ref, number).wait_recv()

    def finish_send(ref, number):
        copy(z_peer((z + 1) % 8), ref, ref, number).wait_send()

    early_send = send_ref.reshape(2, 8, 32, 8, 128).at[0]
    late_send = send_ref.reshape(2, 8, 32, 8, 128).at[1]

    squares, phase_real_0, phase_imag_0 = spread_half(0, zero)
    def early_z(there):
        copy(z_peer(there), early_send.at[there % 2 * 4 + there // 2], mid_a_ref.at[z_slot], 1).start()

    def early_sends(odd):
        @pl.when((z + odd) % 2 == 0)
        def _():
            for d in (4, 2, 6):
                early_z((z + d) % 8)

        @pl.when((z + odd) % 2 == 1)
        def _():
            for d in (3, 5, 1, 7):
                early_z((z + d) % 8)

    transform(0, 0)
    pl.semaphore_wait(barrier, 7 + jnp.where(z == 0, 31, 0))
    early_sends(0)
    transform(0, 2)
    early_sends(1)

    def line_ready(t, _):
        pl.semaphore_signal(round_sem.at[0], inc=1, device_id=plane_peer(t)[0], device_id_type=MESH)
        return 0

    @pl.when(z == 0)
    def _():
        lax.fori_loop(1, 32, line_ready, 0)

    squares, phase_real_1, phase_imag_1 = spread_half(1, squares)
    transform(1, 0)
    transform(1, 2)

    column = lax.broadcasted_iota(jnp.int32, (8, 128), 1)
    sub = lax.broadcasted_iota(jnp.int32, (8, 128), 0)
    turned_real, turned_imag = zero, zero
    for half, phase_real, phase_imag in ((0, phase_real_0, phase_imag_0), (1, phase_real_1, phase_imag_1)):
        angle = (half * 65536 + sub * 256 + slot).astype(jnp.float32) * (2.0 * math.pi / TOTAL)
        cosine, sine = jnp.cos(angle), jnp.sin(angle)
        turned_real = turned_real + (phase_real * cosine + phase_imag * sine)
        turned_imag = turned_imag + (phase_imag * cosine - phase_real * sine)
    lane = lax.broadcasted_iota(jnp.int32, (1, 128), 1)
    row = jnp.zeros((1, 128), jnp.float32)
    for i, value in enumerate((
        squares, jnp.where(column == 1, turned_real, 0.0), jnp.where(column == 1, turned_imag, 0.0),
    )):
        summed = jnp.sum(jnp.sum(value, 0, keepdims=True), 1, keepdims=True)
        row = jnp.where(lane == i, summed, row)
    psum_ref[plane] = row

    @pl.when(z == 0)
    def _():
        pl.semaphore_wait(round_sem.at[0], 31)
        for there in range(1, 8):
            pl.semaphore_signal(round_sem.at[1], inc=1, device_id=z_peer(there), device_id_type=MESH)

    @pl.when(z != 0)
    def _():
        pl.semaphore_wait(round_sem.at[1], 1)

    def plane_bulk(source, target, number):
        def body(t, _):
            peer, there = plane_peer(t)
            copy(peer, source.at[:, there], target.at[:, p_slot], number).start()
            return 0

        lax.fori_loop(1, 32, body, 0)

    def plane_sums(t, _):
        copy(plane_peer(t)[0], psum_ref.at[plane], psum_ref.at[plane], 3).start()
        return 0

    lax.fori_loop(1, 32, plane_sums, 0)
    plane_bulk(late_send, mid_b_ref, 2)
    mid_a_ref[z_slot] = early_send[z_index]
    for i in range(8):
        mid_b_ref[i, p_slot] = late_send[i, plane]

    finish_recv(psum_ref.at[pl.ds(0, 31)], 3)
    total = psum_ref[0]
    for i in range(1, 32):
        total = total + psum_ref[i]
    zsum_ref[z] = total
    for d in range(1, 8):
        copy(z_peer((z + d) % 8), zsum_ref.at[z], zsum_ref.at[z], 0).start()

    finish_recv(mid_b_ref.at[:, pl.ds(0, 31)], 2)

    def late_z(there):
        copy(z_peer(there), mid_b_ref.at[there % 2 * 4 + there // 2], late_ref.at[z_slot], 4).start()

    for there in (0, 1, 2, 3, 4, 5, 6, 7):
        pl.when(there != z)(lambda there=there: late_z(there))

    late_ref[z_slot] = mid_b_ref[z_index]

    finish_recv(mid_a_ref.at[pl.ds(0, 7)], 1)
    plane_bulk(mid_a_ref, early_ref, 5)
    for i in range(8):
        early_ref[i, p_slot] = mid_a_ref[i, plane]

    finish_recv(zsum_ref.at[pl.ds(0, 7)], 0)
    total = zsum_ref[0]
    for i in range(1, 8):
        total = total + zsum_ref[i]
    sums_ref[...] = total
    factor = scale_factor(total[:, 0:1])[1]

    finish_recv(early_ref.at[:, pl.ds(0, 31)], 5)
    place_rows(early_ref.reshape(2048, 128), placed_ref, factor)

    finish_recv(late_ref.at[pl.ds(0, 7)], 4)
    finish_send(zsum_ref.at[pl.ds(0, 7)], 0)
    finish_send(mid_a_ref.at[pl.ds(0, 7)], 1)
    finish_send(mid_b_ref.at[:, pl.ds(0, 31)], 2)
    finish_send(psum_ref.at[pl.ds(0, 31)], 3)
    finish_send(mid_b_ref.at[pl.ds(0, 7)], 4)
    finish_send(early_ref.at[:, pl.ds(0, 31)], 5)


def place_rows(source, target, factor):
    def body(part, _):
        place_part(source, target, factor, part)
        return 0

    lax.fori_loop(0, 4, body, 0)


def place_part(source, target, factor, part):
    for s in range(2):
        for d in range(2):
            block = source[pl.ds(d * 1024 + part * 2 + s, 128, stride=8), :]
            target[pl.ds(part * 512 + d * 2 + s, 128, stride=4), :] = block.T * factor


def place_kernel(placed_ref, late_ref, sums_ref, out_hbm, checks_ref, buffer_ref, sems):
    copies = []

    def move(source, first, size, number):
        copies.append(pltpu.make_async_copy(source, out_hbm.at[pl.ds(first, size)], sems.at[number]))
        copies[-1].start()

    for f in range(2):
        move(placed_ref.at[pl.ds(f * 1024, 1024)], f * 2048, 1024, f)
    sums = sums_ref[...]
    mean_square, factor = scale_factor(sums[:, 0:1])
    for part in range(4):
        place_part(late_ref, buffer_ref, factor, part)
        first = part // 2 * 2048 + 1024 + part % 2 * 512
        move(buffer_ref.at[pl.ds(part * 512, 512)], first, 512, 2 + part)
    scale = factor * (math.sqrt(WINDOW) / math.sqrt(TOTAL))
    checks_ref[0] = mean_square[0, 0]
    for i in (1, 2):
        checks_ref[i] = (sums[:, i : i + 1] * scale)[0, 0]
    for moved in copies:
        moved.wait()


def per_device(amplitudes):
    rows = amplitudes.reshape(2, 2048, 128).transpose(1, 0, 2).reshape(256, 2, 8, 128)
    vmem = pl.BlockSpec(memory_space=pltpu.VMEM)
    hbm = pl.BlockSpec(memory_space=pltpu.HBM)
    f32, bf16 = jnp.float32, jnp.bfloat16
    placed, late, sums = pl.pallas_call(
        exchange_kernel,
        out_shape=(
            jax.ShapeDtypeStruct((2048, 128), f32),
            jax.ShapeDtypeStruct((8, 32, 8, 128), f32),
            jax.ShapeDtypeStruct((1, 128), f32),
        ),
        in_specs=[hbm],
        out_specs=(vmem, vmem, vmem),
        scratch_shapes=[
            pltpu.VMEM((2, 8, 33, 8, 128), f32),
            pltpu.VMEM((256, 256), bf16),
            pltpu.VMEM((256, 256), bf16),
            pltpu.VMEM((4, 256, 256), bf16),
            pltpu.VMEM((4, 256, 256), bf16),
            pltpu.VMEM((2, 2048, 128), f32),
            pltpu.VMEM((8, 32, 8, 128), f32),
            pltpu.VMEM((8, 32, 8, 128), f32),
            pltpu.VMEM((8, 32, 8, 128), f32),
            pltpu.VMEM((8, 1, 128), f32),
            pltpu.VMEM((32, 1, 128), f32),
            pltpu.SemaphoreType.DMA((2, 8)),
            pltpu.SemaphoreType.DMA((6,)),
            pltpu.SemaphoreType.DMA((6,)),
            pltpu.SemaphoreType.REGULAR((2,)),
        ],
        compiler_params=pltpu.CompilerParams(
            collective_id=1, has_side_effects=True, vmem_limit_bytes=51 * 1024 * 1024
        ),
    )(rows)
    out, checks = pl.pallas_call(
        place_kernel,
        out_shape=(
            jax.ShapeDtypeStruct((4096, 128), f32),
            jax.ShapeDtypeStruct((3,), f32),
        ),
        in_specs=[vmem, vmem, vmem],
        out_specs=(hbm, pl.BlockSpec(memory_space=pltpu.SMEM)),
        scratch_shapes=[pltpu.VMEM((2048, 128), f32), pltpu.SemaphoreType.DMA((6,))],
        compiler_params=pltpu.CompilerParams(vmem_limit_bytes=16 * 1024 * 1024),
    )(placed, late.reshape(2048, 128), sums)
    transformed = out.reshape(2048, 2, 128).transpose(1, 0, 2).reshape(2, AMP_DEV)
    return transformed, checks


def solution(mesh):
    return jax.shard_map(
        per_device,
        mesh=mesh,
        in_specs=(P(None, AXES),),
        out_specs=(P(None, AXES), P()),
        check_vma=False,
    )
```

```python
import math

import jax
import jax.numpy as jnp
from jax import lax
from jax.experimental import pallas as pl
from jax.experimental.pallas import tpu as pltpu
from jax.sharding import PartitionSpec as P

MESH = pl.DeviceIdType.MESH
AXES = ("outer", "inner")
AMP_DEV = 262144
DEVICES = 256
TOTAL = AMP_DEV * DEVICES
WINDOW = 512
PITCH = 264
SPAN = 8 * PITCH


def reverse_bits(value, count):
    result = 0
    for bit in range(count):
        result = result + (value // 2**bit) % 2 * 2 ** (count - 1 - bit)
    return result


def scale_factor(squares):
    mean_square = squares / TOTAL
    return mean_square, lax.rsqrt(mean_square + 1e-06)


def exchange_kernel(
    x_hbm, placed_ref, late_ref, sums_ref,
    a_ref, high_ref, low_ref, bh_ref, bl_ref,
    send_ref, mid_a_ref, mid_b_ref, early_ref, zsum_ref, psum_ref,
    load_sem, send_sem, recv_sem, round_sem,
):
    loads = [
        [
            pltpu.make_async_copy(
                x_hbm.at[pl.ds(32 * top, 32), half],
                a_ref.at[half, reverse_bits(top, 3), pl.ds(0, 32)],
                load_sem.at[half, top],
            )
            for top in range(8)
        ]
        for half in range(2)
    ]
    for load in loads[0]:
        load.start()

    outer, inner = lax.axis_index("outer"), lax.axis_index("inner")
    y, c, x, z = outer // 2, outer % 2, inner // 8, inner % 8
    plane = outer * 4 + x
    z_slot, p_slot = reverse_bits(z, 3), reverse_bits(plane, 5)
    z_index = z % 2 * 4 + z // 2
    slot = z_slot * 32 + p_slot

    def z_peer(there):
        return (outer, x * 8 + there)

    def plane_peer(t):
        dx, dy, dc = t % 4, (t % 4 + t // 4) % 4, (t + t // 16) % 2
        there_outer, there_x = (y + dy) % 4 * 2 + (c + dc) % 2, (x + dx) % 4
        return (there_outer, there_x * 8 + z), there_outer * 4 + there_x

    barrier = pltpu.get_barrier_semaphore()
    for d in range(1, 8):
        pl.semaphore_signal(barrier, inc=1, device_id=z_peer((z + d) % 8), device_id_type=MESH)

    def greet(t, _):
        pl.semaphore_signal(barrier, inc=1, device_id=plane_peer(t)[0], device_id_type=MESH)
        return 0

    @pl.when(z == 0)
    def _():
        lax.fori_loop(1, 32, greet, 0)

    lane = lax.broadcasted_iota(jnp.int32, (128, 128), 1)
    row = lax.broadcasted_iota(jnp.int32, (128, 128), 0)
    frequency = (row & 31) * 4 + (row >> 5)
    angle = ((frequency * lane) & 127).astype(jnp.float32) * (2.0 * math.pi / 128)
    for value, places in (
        (jnp.cos(angle) * WINDOW**-0.5, ((0, 0, 1.0), (1, 1, 1.0))),
        (jnp.sin(angle) * WINDOW**-0.5, ((1, 0, 1.0), (0, 1, -1.0))),
    ):
        high = value.astype(jnp.bfloat16)
        low = (value - high.astype(jnp.float32)).astype(jnp.bfloat16)
        for i, j, sign in places:
            high_ref[128 * i : 128 * i + 128, 128 * j : 128 * j + 128] = high * jnp.bfloat16(sign)
            low_ref[128 * i : 128 * i + 128, 128 * j : 128 * j + 128] = low * jnp.bfloat16(sign)
    lane = lax.broadcasted_iota(jnp.int32, (16, 128), 1)
    twiddles = []
    for g in (1, 2, 3):
        angle = (lane * g).astype(jnp.float32) * (2.0 * math.pi / WINDOW)
        twiddles.append((jnp.cos(angle), jnp.sin(angle)))

    step = 2.0 * math.pi * 2048 / TOTAL
    cos_step, sin_step = math.cos(step), math.sin(step)
    a_rows = a_ref.reshape(2 * SPAN, 128)
    zero = jnp.zeros((8, 128), jnp.float32)

    def spread_half(half, squares):
        for load in loads[half]:
            load.wait()
        if half == 0:
            for load in loads[1]:
                load.start()

        def spread(turn, carry):
            squares, phase_real, phase_imag = carry
            h = 15 - turn
            middle = reverse_bits(h, 4)
            parts = [
                [
                    a_rows[pl.ds(half * SPAN + (middle + 16 * b) * 8 + q, 8, stride=PITCH), :]
                    for q in range(8)
                ]
                for b in range(2)
            ]
            for b in (1, 0):
                phase_real, phase_imag = (
                    phase_real * cos_step + phase_imag * sin_step + parts[b][0],
                    phase_imag * cos_step - phase_real * sin_step + parts[b][1],
                )
                for q in range(8):
                    squares = squares + parts[b][q] * parts[b][q]
            v = [jnp.concatenate([parts[0][q], parts[1][q]], 0) for q in range(8)]
            real, imag = v[0::2], v[1::2]
            s02r, s02i = real[0] + real[2], imag[0] + imag[2]
            d02r, d02i = real[0] - real[2], imag[0] - imag[2]
            s13r, s13i = real[1] + real[3], imag[1] + imag[3]
            d13r, d13i = real[1] - real[3], imag[1] - imag[3]
            u = [
                (s02r + s13r, s02i + s13i),
                (d02r - d13i, d02i + d13r),
                (s02r - s13r, s02i - s13i),
                (d02r + d13i, d02i - d13r),
            ]
            rows = pl.ds(pl.multiple_of(h * 16, 16), 16)
            for g in range(4):
                ur, ui = u[g]
                if g:
                    cosine, sine = twiddles[g - 1]
                    ur, ui = ur * cosine - ui * sine, ur * sine + ui * cosine
                for s, value in ((0, ur), (1, ui)):
                    high = value.astype(jnp.bfloat16)
                    low = (value - high.astype(jnp.float32)).astype(jnp.bfloat16)
                    bh_ref[g, rows, 128 * s : 128 * s + 128] = high
                    bl_ref[g, rows, 128 * s : 128 * s + 128] = low
            return squares, phase_real, phase_imag

        return lax.fori_loop(0, 16, spread, (squares, zero, zero))

    def transform(half, first):
        for f in range(2):
            bh, bl = bh_ref[first + f], bl_ref[first + f]
            dims = (((1,), (1,)), ((), ()))
            out = (
                lax.dot_general(high_ref[...], bh, dims, preferred_element_type=jnp.float32)
                + lax.dot_general(high_ref[...], bl, dims, preferred_element_type=jnp.float32)
                + lax.dot_general(low_ref[...], bh, dims, preferred_element_type=jnp.float32)
            )
            for k in range(2):
                for s in range(2):
                    place = pl.ds(first // 2 * 1024 + f * 4 + k * 2 + s, 128, stride=8)
                    send_ref[half, place, :] = out[128 * s : 128 * s + 128, 128 * k : 128 * k + 128]

    def copy(peer, source, target, number):
        return pltpu.make_async_remote_copy(
            src_ref=source,
            dst_ref=target,
            send_sem=send_sem.at[number],
            recv_sem=recv_sem.at[number],
            device_id=peer,
            device_id_type=MESH,
        )

    def finish_recv(ref, number):
        copy(z_peer((z + 1) % 8), ref, ref, number).wait_recv()

    def finish_send(ref, number):
        copy(z_peer((z + 1) % 8), ref, ref, number).wait_send()

    early_send = send_ref.reshape(2, 8, 32, 8, 128).at[0]
    late_send = send_ref.reshape(2, 8, 32, 8, 128).at[1]

    squares, phase_real_0, phase_imag_0 = spread_half(0, zero)
    def early_z(there):
        copy(z_peer(there), early_send.at[there % 2 * 4 + there // 2], mid_a_ref.at[z_slot], 1).start()

    def early_sends(odd):
        @pl.when((z + odd) % 2 == 0)
        def _():
            for d in (4, 2, 6):
                early_z((z + d) % 8)

        @pl.when((z + odd) % 2 == 1)
        def _():
            for d in (3, 5, 1, 7):
                early_z((z + d) % 8)

    transform(0, 0)
    pl.semaphore_wait(barrier, 7 + jnp.where(z == 0, 31, 0))
    early_sends(0)
    transform(0, 2)
    early_sends(1)

    def line_ready(t, _):
        pl.semaphore_signal(round_sem.at[0], inc=1, device_id=plane_peer(t)[0], device_id_type=MESH)
        return 0

    @pl.when(z == 0)
    def _():
        lax.fori_loop(1, 32, line_ready, 0)

    squares, phase_real_1, phase_imag_1 = spread_half(1, squares)
    transform(1, 0)
    transform(1, 2)

    column = lax.broadcasted_iota(jnp.int32, (8, 128), 1)
    sub = lax.broadcasted_iota(jnp.int32, (8, 128), 0)
    turned_real, turned_imag = zero, zero
    for half, phase_real, phase_imag in ((0, phase_real_0, phase_imag_0), (1, phase_real_1, phase_imag_1)):
        angle = (half * 65536 + sub * 256 + slot).astype(jnp.float32) * (2.0 * math.pi / TOTAL)
        cosine, sine = jnp.cos(angle), jnp.sin(angle)
        turned_real = turned_real + (phase_real * cosine + phase_imag * sine)
        turned_imag = turned_imag + (phase_imag * cosine - phase_real * sine)
    lane = lax.broadcasted_iota(jnp.int32, (1, 128), 1)
    row = jnp.zeros((1, 128), jnp.float32)
    for i, value in enumerate((
        squares, jnp.where(column == 1, turned_real, 0.0), jnp.where(column == 1, turned_imag, 0.0),
    )):
        summed = jnp.sum(jnp.sum(value, 0, keepdims=True), 1, keepdims=True)
        row = jnp.where(lane == i, summed, row)
    psum_ref[plane] = row

    @pl.when(z == 0)
    def _():
        pl.semaphore_wait(round_sem.at[0], 31)
        for there in range(1, 8):
            pl.semaphore_signal(round_sem.at[1], inc=1, device_id=z_peer(there), device_id_type=MESH)

    @pl.when(z != 0)
    def _():
        pl.semaphore_wait(round_sem.at[1], 1)

    def plane_bulk(source, target, number):
        def body(t, _):
            peer, there = plane_peer(t)
            copy(peer, source.at[:, there], target.at[:, p_slot], number).start()
            return 0

        lax.fori_loop(1, 32, body, 0)

    def plane_sums(t, _):
        copy(plane_peer(t)[0], psum_ref.at[plane], psum_ref.at[plane], 3).start()
        return 0

    lax.fori_loop(1, 32, plane_sums, 0)
    plane_bulk(late_send, mid_b_ref, 2)
    mid_a_ref[z_slot] = early_send[z_index]
    for i in range(8):
        mid_b_ref[i, p_slot] = late_send[i, plane]

    finish_recv(psum_ref.at[pl.ds(0, 31)], 3)
    total = psum_ref[0]
    for i in range(1, 32):
        total = total + psum_ref[i]
    zsum_ref[z] = total
    for d in range(1, 8):
        copy(z_peer((z + d) % 8), zsum_ref.at[z], zsum_ref.at[z], 0).start()

    finish_recv(mid_b_ref.at[:, pl.ds(0, 31)], 2)

    def late_z(there):
        copy(z_peer(there), mid_b_ref.at[there % 2 * 4 + there // 2], late_ref.at[z_slot], 4).start()

    for there in (0, 1, 2, 3, 4, 5, 6, 7):
        pl.when(there != z)(lambda there=there: late_z(there))

    late_ref[z_slot] = mid_b_ref[z_index]

    finish_recv(mid_a_ref.at[pl.ds(0, 7)], 1)
    plane_bulk(mid_a_ref, early_ref, 5)
    for i in range(8):
        early_ref[i, p_slot] = mid_a_ref[i, plane]

    finish_recv(zsum_ref.at[pl.ds(0, 7)], 0)
    total = zsum_ref[0]
    for i in range(1, 8):
        total = total + zsum_ref[i]
    sums_ref[...] = total
    factor = scale_factor(total[:, 0:1])[1]

    finish_recv(early_ref.at[:, pl.ds(0, 31)], 5)
    place_rows(early_ref.reshape(2048, 128), placed_ref, factor)

    finish_recv(late_ref.at[pl.ds(0, 7)], 4)
    finish_send(zsum_ref.at[pl.ds(0, 7)], 0)
    finish_send(mid_a_ref.at[pl.ds(0, 7)], 1)
    finish_send(mid_b_ref.at[:, pl.ds(0, 31)], 2)
    finish_send(psum_ref.at[pl.ds(0, 31)], 3)
    finish_send(mid_b_ref.at[pl.ds(0, 7)], 4)
    finish_send(early_ref.at[:, pl.ds(0, 31)], 5)


def place_rows(source, target, factor):
    def body(part, _):
        place_part(source, target, factor, part)
        return 0

    lax.fori_loop(0, 4, body, 0)


def place_part(source, target, factor, part):
    for s in range(2):
        for d in range(2):
            block = source[pl.ds(d * 1024 + part * 2 + s, 128, stride=8), :]
            target[pl.ds(part * 512 + d * 2 + s, 128, stride=4), :] = block.T * factor


def place_kernel(placed_ref, late_ref, sums_ref, out_hbm, checks_hbm, buffer_ref, checks_ref, sems):
    copies = []

    def move(source, first, size, number):
        copies.append(pltpu.make_async_copy(source, out_hbm.at[pl.ds(first, size)], sems.at[number]))
        copies[-1].start()

    for f in range(2):
        move(placed_ref.at[pl.ds(f * 1024, 1024)], f * 2048, 1024, f)
    sums = sums_ref[...]
    mean_square, factor = scale_factor(sums[:, 0:1])
    scale = factor * (math.sqrt(WINDOW) / math.sqrt(TOTAL))
    checks_ref[0] = mean_square[0, 0]
    for i in (1, 2):
        checks_ref[i] = (sums[:, i : i + 1] * scale)[0, 0]
    copies.append(pltpu.make_async_copy(checks_ref, checks_hbm, sems.at[6]))
    copies[-1].start()
    for part in range(4):
        place_part(late_ref, buffer_ref, factor, part)
        first = part // 2 * 2048 + 1024 + part % 2 * 512
        move(buffer_ref.at[pl.ds(part * 512, 512)], first, 512, 2 + part)
    for moved in copies:
        moved.wait()


def per_device(amplitudes):
    rows = amplitudes.reshape(2, 2048, 128).transpose(1, 0, 2).reshape(256, 2, 8, 128)
    vmem = pl.BlockSpec(memory_space=pltpu.VMEM)
    hbm = pl.BlockSpec(memory_space=pltpu.HBM)
    f32, bf16 = jnp.float32, jnp.bfloat16
    placed, late, sums = pl.pallas_call(
        exchange_kernel,
        out_shape=(
            jax.ShapeDtypeStruct((2048, 128), f32),
            jax.ShapeDtypeStruct((8, 32, 8, 128), f32),
            jax.ShapeDtypeStruct((1, 128), f32),
        ),
        in_specs=[hbm],
        out_specs=(vmem, vmem, vmem),
        scratch_shapes=[
            pltpu.VMEM((2, 8, 33, 8, 128), f32),
            pltpu.VMEM((256, 256), bf16),
            pltpu.VMEM((256, 256), bf16),
            pltpu.VMEM((4, 256, 256), bf16),
            pltpu.VMEM((4, 256, 256), bf16),
            pltpu.VMEM((2, 2048, 128), f32),
            pltpu.VMEM((8, 32, 8, 128), f32),
            pltpu.VMEM((8, 32, 8, 128), f32),
            pltpu.VMEM((8, 32, 8, 128), f32),
            pltpu.VMEM((8, 1, 128), f32),
            pltpu.VMEM((32, 1, 128), f32),
            pltpu.SemaphoreType.DMA((2, 8)),
            pltpu.SemaphoreType.DMA((6,)),
            pltpu.SemaphoreType.DMA((6,)),
            pltpu.SemaphoreType.REGULAR((2,)),
        ],
        compiler_params=pltpu.CompilerParams(
            collective_id=1, has_side_effects=True, vmem_limit_bytes=51 * 1024 * 1024
        ),
    )(rows)
    out, checks = pl.pallas_call(
        place_kernel,
        out_shape=(
            jax.ShapeDtypeStruct((4096, 128), f32),
            jax.ShapeDtypeStruct((3,), f32),
        ),
        in_specs=[vmem, vmem, vmem],
        out_specs=(hbm, hbm),
        scratch_shapes=[
            pltpu.VMEM((2048, 128), f32),
            pltpu.SMEM((3,), f32),
            pltpu.SemaphoreType.DMA((7,)),
        ],
        compiler_params=pltpu.CompilerParams(vmem_limit_bytes=16 * 1024 * 1024),
    )(placed, late.reshape(2048, 128), sums)
    transformed = out.reshape(2048, 2, 128).transpose(1, 0, 2).reshape(2, AMP_DEV)
    return transformed, checks


def solution(mesh):
    return jax.shard_map(
        per_device,
        mesh=mesh,
        in_specs=(P(None, AXES),),
        out_specs=(P(None, AXES), P()),
        check_vma=False,
    )
```

```python
import math

import jax
import jax.numpy as jnp
from jax import lax
from jax.experimental import pallas as pl
from jax.experimental.pallas import tpu as pltpu
from jax.sharding import PartitionSpec as P

MESH = pl.DeviceIdType.MESH
AXES = ("outer", "inner")
AMP_DEV = 262144
DEVICES = 256
TOTAL = AMP_DEV * DEVICES
WINDOW = 512
PITCH = 264
SPAN = 8 * PITCH


def reverse_bits(value, count):
    result = 0
    for bit in range(count):
        result = result + (value // 2**bit) % 2 * 2 ** (count - 1 - bit)
    return result


def scale_factor(squares):
    mean_square = squares / TOTAL
    return mean_square, lax.rsqrt(mean_square + 1e-06)


def exchange_kernel(
    x_hbm, placed_ref, late_ref, sums_ref,
    a_ref, high_ref, low_ref, bh_ref, bl_ref,
    send_ref, mid_a_ref, mid_b_ref, early_ref, zsum_ref, psum_ref,
    load_sem, send_sem, recv_sem, round_sem,
):
    loads = [
        [
            pltpu.make_async_copy(
                x_hbm.at[pl.ds(32 * top, 32), half],
                a_ref.at[half, reverse_bits(top, 3), pl.ds(0, 32)],
                load_sem.at[half, top],
            )
            for top in range(8)
        ]
        for half in range(2)
    ]
    for load in loads[0]:
        load.start()

    outer, inner = lax.axis_index("outer"), lax.axis_index("inner")
    y, c, x, z = outer // 2, outer % 2, inner // 8, inner % 8
    plane = outer * 4 + x
    z_slot, p_slot = reverse_bits(z, 3), reverse_bits(plane, 5)
    z_index = z % 2 * 4 + z // 2
    slot = z_slot * 32 + p_slot

    def z_peer(there):
        return (outer, x * 8 + there)

    def plane_peer(t):
        dx, dy, dc = t % 4, (t % 4 + t // 4) % 4, (t + t // 16) % 2
        there_outer, there_x = (y + dy) % 4 * 2 + (c + dc) % 2, (x + dx) % 4
        return (there_outer, there_x * 8 + z), there_outer * 4 + there_x

    barrier = pltpu.get_barrier_semaphore()
    for d in range(1, 8):
        pl.semaphore_signal(barrier, inc=1, device_id=z_peer((z + d) % 8), device_id_type=MESH)

    def greet(t, _):
        pl.semaphore_signal(barrier, inc=1, device_id=plane_peer(t)[0], device_id_type=MESH)
        return 0

    @pl.when(z == 0)
    def _():
        lax.fori_loop(1, 32, greet, 0)

    lane = lax.broadcasted_iota(jnp.int32, (128, 128), 1)
    row = lax.broadcasted_iota(jnp.int32, (128, 128), 0)
    frequency = (row & 31) * 4 + (row >> 5)
    angle = ((frequency * lane) & 127).astype(jnp.float32) * (2.0 * math.pi / 128)
    for value, places in (
        (jnp.cos(angle) * WINDOW**-0.5, ((0, 0, 1.0), (1, 1, 1.0))),
        (jnp.sin(angle) * WINDOW**-0.5, ((1, 0, 1.0), (0, 1, -1.0))),
    ):
        high = value.astype(jnp.bfloat16)
        low = (value - high.astype(jnp.float32)).astype(jnp.bfloat16)
        for i, j, sign in places:
            high_ref[128 * i : 128 * i + 128, 128 * j : 128 * j + 128] = high * jnp.bfloat16(sign)
            low_ref[128 * i : 128 * i + 128, 128 * j : 128 * j + 128] = low * jnp.bfloat16(sign)
    lane = lax.broadcasted_iota(jnp.int32, (16, 128), 1)
    twiddles = []
    for g in (1, 2, 3):
        angle = (lane * g).astype(jnp.float32) * (2.0 * math.pi / WINDOW)
        twiddles.append((jnp.cos(angle), jnp.sin(angle)))

    step = 2.0 * math.pi * 2048 / TOTAL
    cos_step, sin_step = math.cos(step), math.sin(step)
    a_rows = a_ref.reshape(2 * SPAN, 128)
    zero = jnp.zeros((8, 128), jnp.float32)

    def spread_half(half, squares):
        for load in loads[half]:
            load.wait()
        if half == 0:
            for load in loads[1]:
                load.start()

        def spread(turn, carry):
            squares, phase_real, phase_imag = carry
            h = 15 - turn
            middle = reverse_bits(h, 4)
            parts = [
                [
                    a_rows[pl.ds(half * SPAN + (middle + 16 * b) * 8 + q, 8, stride=PITCH), :]
                    for q in range(8)
                ]
                for b in range(2)
            ]
            for b in (1, 0):
                phase_real, phase_imag = (
                    phase_real * cos_step + phase_imag * sin_step + parts[b][0],
                    phase_imag * cos_step - phase_real * sin_step + parts[b][1],
                )
                for q in range(8):
                    squares = squares + parts[b][q] * parts[b][q]
            v = [jnp.concatenate([parts[0][q], parts[1][q]], 0) for q in range(8)]
            real, imag = v[0::2], v[1::2]
            s02r, s02i = real[0] + real[2], imag[0] + imag[2]
            d02r, d02i = real[0] - real[2], imag[0] - imag[2]
            s13r, s13i = real[1] + real[3], imag[1] + imag[3]
            d13r, d13i = real[1] - real[3], imag[1] - imag[3]
            u = [
                (s02r + s13r, s02i + s13i),
                (d02r - d13i, d02i + d13r),
                (s02r - s13r, s02i - s13i),
                (d02r + d13i, d02i - d13r),
            ]
            rows = pl.ds(pl.multiple_of(h * 16, 16), 16)
            for g in range(4):
                ur, ui = u[g]
                if g:
                    cosine, sine = twiddles[g - 1]
                    ur, ui = ur * cosine - ui * sine, ur * sine + ui * cosine
                for s, value in ((0, ur), (1, ui)):
                    high = value.astype(jnp.bfloat16)
                    low = (value - high.astype(jnp.float32)).astype(jnp.bfloat16)
                    bh_ref[g, rows, 128 * s : 128 * s + 128] = high
                    bl_ref[g, rows, 128 * s : 128 * s + 128] = low
            return squares, phase_real, phase_imag

        return lax.fori_loop(0, 16, spread, (squares, zero, zero))

    def transform(half, first):
        for f in range(2):
            bh, bl = bh_ref[first + f], bl_ref[first + f]
            dims = (((1,), (1,)), ((), ()))
            out = (
                lax.dot_general(high_ref[...], bh, dims, preferred_element_type=jnp.float32)
                + lax.dot_general(high_ref[...], bl, dims, preferred_element_type=jnp.float32)
                + lax.dot_general(low_ref[...], bh, dims, preferred_element_type=jnp.float32)
            )
            for k in range(2):
                for s in range(2):
                    place = pl.ds(first // 2 * 1024 + f * 4 + k * 2 + s, 128, stride=8)
                    send_ref[half, place, :] = out[128 * s : 128 * s + 128, 128 * k : 128 * k + 128]

    def copy(peer, source, target, number):
        return pltpu.make_async_remote_copy(
            src_ref=source,
            dst_ref=target,
            send_sem=send_sem.at[number],
            recv_sem=recv_sem.at[number],
            device_id=peer,
            device_id_type=MESH,
        )

    def finish_recv(ref, number):
        copy(z_peer((z + 1) % 8), ref, ref, number).wait_recv()

    def finish_send(ref, number):
        copy(z_peer((z + 1) % 8), ref, ref, number).wait_send()

    early_send = send_ref.reshape(2, 8, 32, 8, 128).at[0]
    late_send = send_ref.reshape(2, 2, 4, 32, 8, 128).at[1]

    squares, phase_real_0, phase_imag_0 = spread_half(0, zero)
    def early_z(there):
        copy(z_peer(there), early_send.at[there % 2 * 4 + there // 2], mid_a_ref.at[z_slot], 1).start()

    def early_sends(odd):
        @pl.when((z + odd) % 2 == 0)
        def _():
            for d in (4, 2, 6):
                early_z((z + d) % 8)

        @pl.when((z + odd) % 2 == 1)
        def _():
            for d in (3, 5, 1, 7):
                early_z((z + d) % 8)

    transform(0, 0)
    pl.semaphore_wait(barrier, 7 + jnp.where(z == 0, 31, 0))
    early_sends(0)
    transform(0, 2)
    early_sends(1)

    def line_ready(t, _):
        pl.semaphore_signal(round_sem.at[0], inc=1, device_id=plane_peer(t)[0], device_id_type=MESH)
        return 0

    @pl.when(z == 0)
    def _():
        lax.fori_loop(1, 32, line_ready, 0)

    squares, phase_real_1, phase_imag_1 = spread_half(1, squares)
    transform(1, 0)
    transform(1, 2)

    column = lax.broadcasted_iota(jnp.int32, (8, 128), 1)
    sub = lax.broadcasted_iota(jnp.int32, (8, 128), 0)
    turned_real, turned_imag = zero, zero
    for half, phase_real, phase_imag in ((0, phase_real_0, phase_imag_0), (1, phase_real_1, phase_imag_1)):
        angle = (half * 65536 + sub * 256 + slot).astype(jnp.float32) * (2.0 * math.pi / TOTAL)
        cosine, sine = jnp.cos(angle), jnp.sin(angle)
        turned_real = turned_real + (phase_real * cosine + phase_imag * sine)
        turned_imag = turned_imag + (phase_imag * cosine - phase_real * sine)
    lane = lax.broadcasted_iota(jnp.int32, (1, 128), 1)
    row = jnp.zeros((1, 128), jnp.float32)
    for i, value in enumerate((
        squares, jnp.where(column == 1, turned_real, 0.0), jnp.where(column == 1, turned_imag, 0.0),
    )):
        summed = jnp.sum(jnp.sum(value, 0, keepdims=True), 1, keepdims=True)
        row = jnp.where(lane == i, summed, row)
    psum_ref[plane] = row

    @pl.when(z == 0)
    def _():
        pl.semaphore_wait(round_sem.at[0], 31)
        for there in range(1, 8):
            pl.semaphore_signal(round_sem.at[1], inc=1, device_id=z_peer(there), device_id_type=MESH)

    @pl.when(z != 0)
    def _():
        pl.semaphore_wait(round_sem.at[1], 1)

    def plane_bulk(source, target, number):
        def body(t, _):
            peer, there = plane_peer(t)
            copy(peer, source.at[:, there], target.at[:, p_slot], number).start()
            return 0

        lax.fori_loop(1, 32, body, 0)

    def plane_sums(t, _):
        copy(plane_peer(t)[0], psum_ref.at[plane], psum_ref.at[plane], 3).start()
        return 0

    lax.fori_loop(1, 32, plane_sums, 0)

    def late_bulk(part):
        def body(t, _):
            peer, there = plane_peer(t)
            source = late_send.at[:, pl.ds(2 * part, 2), there]
            copy(peer, source, mid_b_ref.at[:, pl.ds(2 * part, 2), p_slot], 2 + 4 * part).start()
            return 0

        lax.fori_loop(1, 32, body, 0)

    late_bulk(0)
    late_bulk(1)
    mid_a_ref[z_slot] = early_send[z_index]
    for i in range(8):
        mid_b_ref[i // 4, i % 4, p_slot] = late_send[i // 4, i % 4, plane]

    finish_recv(psum_ref.at[pl.ds(0, 31)], 3)
    total = psum_ref[0]
    for i in range(1, 32):
        total = total + psum_ref[i]
    zsum_ref[z] = total
    for d in range(1, 8):
        copy(z_peer((z + d) % 8), zsum_ref.at[z], zsum_ref.at[z], 0).start()

    def late_z(there):
        copy(z_peer(there), mid_b_ref.at[there % 2, there // 2], late_ref.at[z_slot], 4).start()

    for part in range(2):
        finish_recv(mid_b_ref.at[:, pl.ds(0, 2), pl.ds(0, 31)], 2 + 4 * part)
        for there in (0, 1, 2, 3, 7, 4, 6, 5)[4 * part : 4 * part + 4]:
            pl.when(there != z)(lambda there=there: late_z(there))

    late_ref[z_slot] = mid_b_ref[z % 2, z // 2]

    finish_recv(mid_a_ref.at[pl.ds(0, 7)], 1)
    plane_bulk(mid_a_ref, early_ref, 5)
    for i in range(8):
        early_ref[i, p_slot] = mid_a_ref[i, plane]

    finish_recv(zsum_ref.at[pl.ds(0, 7)], 0)
    total = zsum_ref[0]
    for i in range(1, 8):
        total = total + zsum_ref[i]
    sums_ref[...] = total
    factor = scale_factor(total[:, 0:1])[1]

    finish_recv(early_ref.at[:, pl.ds(0, 31)], 5)
    place_rows(early_ref.reshape(2048, 128), placed_ref, factor)

    finish_recv(late_ref.at[pl.ds(0, 7)], 4)
    finish_send(zsum_ref.at[pl.ds(0, 7)], 0)
    finish_send(mid_a_ref.at[pl.ds(0, 7)], 1)
    finish_send(mid_b_ref.at[:, pl.ds(0, 2), pl.ds(0, 31)], 2)
    finish_send(mid_b_ref.at[:, pl.ds(0, 2), pl.ds(0, 31)], 6)
    finish_send(psum_ref.at[pl.ds(0, 31)], 3)
    finish_send(late_ref.at[pl.ds(0, 7)], 4)
    finish_send(early_ref.at[:, pl.ds(0, 31)], 5)


def place_rows(source, target, factor):
    def body(part, _):
        place_part(source, target, factor, part)
        return 0

    lax.fori_loop(0, 4, body, 0)


def place_part(source, target, factor, part):
    for s in range(2):
        for d in range(2):
            block = source[pl.ds(d * 1024 + part * 2 + s, 128, stride=8), :]
            target[pl.ds(part * 512 + d * 2 + s, 128, stride=4), :] = block.T * factor


def place_kernel(placed_ref, late_ref, sums_ref, out_hbm, checks_hbm, buffer_ref, checks_ref, sems):
    copies = []

    def move(source, first, size, number):
        copies.append(pltpu.make_async_copy(source, out_hbm.at[pl.ds(first, size)], sems.at[number]))
        copies[-1].start()

    for f in range(2):
        move(placed_ref.at[pl.ds(f * 1024, 1024)], f * 2048, 1024, f)
    sums = sums_ref[...]
    mean_square, factor = scale_factor(sums[:, 0:1])
    scale = factor * (math.sqrt(WINDOW) / math.sqrt(TOTAL))
    checks_ref[0] = mean_square[0, 0]
    for i in (1, 2):
        checks_ref[i] = (sums[:, i : i + 1] * scale)[0, 0]
    copies.append(pltpu.make_async_copy(checks_ref, checks_hbm, sems.at[6]))
    copies[-1].start()
    for part in range(4):
        place_part(late_ref, buffer_ref, factor, part)
        first = part // 2 * 2048 + 1024 + part % 2 * 512
        move(buffer_ref.at[pl.ds(part * 512, 512)], first, 512, 2 + part)
    for moved in copies:
        moved.wait()


def per_device(amplitudes):
    rows = amplitudes.reshape(2, 2048, 128).transpose(1, 0, 2).reshape(256, 2, 8, 128)
    vmem = pl.BlockSpec(memory_space=pltpu.VMEM)
    hbm = pl.BlockSpec(memory_space=pltpu.HBM)
    f32, bf16 = jnp.float32, jnp.bfloat16
    placed, late, sums = pl.pallas_call(
        exchange_kernel,
        out_shape=(
            jax.ShapeDtypeStruct((2048, 128), f32),
            jax.ShapeDtypeStruct((8, 32, 8, 128), f32),
            jax.ShapeDtypeStruct((1, 128), f32),
        ),
        in_specs=[hbm],
        out_specs=(vmem, vmem, vmem),
        scratch_shapes=[
            pltpu.VMEM((2, 8, 33, 8, 128), f32),
            pltpu.VMEM((256, 256), bf16),
            pltpu.VMEM((256, 256), bf16),
            pltpu.VMEM((4, 256, 256), bf16),
            pltpu.VMEM((4, 256, 256), bf16),
            pltpu.VMEM((2, 2048, 128), f32),
            pltpu.VMEM((8, 32, 8, 128), f32),
            pltpu.VMEM((2, 4, 32, 8, 128), f32),
            pltpu.VMEM((8, 32, 8, 128), f32),
            pltpu.VMEM((8, 1, 128), f32),
            pltpu.VMEM((32, 1, 128), f32),
            pltpu.SemaphoreType.DMA((2, 8)),
            pltpu.SemaphoreType.DMA((7,)),
            pltpu.SemaphoreType.DMA((7,)),
            pltpu.SemaphoreType.REGULAR((2,)),
        ],
        compiler_params=pltpu.CompilerParams(
            collective_id=1, has_side_effects=True, vmem_limit_bytes=51 * 1024 * 1024
        ),
    )(rows)
    out, checks = pl.pallas_call(
        place_kernel,
        out_shape=(
            jax.ShapeDtypeStruct((4096, 128), f32),
            jax.ShapeDtypeStruct((3,), f32),
        ),
        in_specs=[vmem, vmem, vmem],
        out_specs=(hbm, hbm),
        scratch_shapes=[
            pltpu.VMEM((2048, 128), f32),
            pltpu.SMEM((3,), f32),
            pltpu.SemaphoreType.DMA((7,)),
        ],
        compiler_params=pltpu.CompilerParams(vmem_limit_bytes=16 * 1024 * 1024),
    )(placed, late.reshape(2048, 128), sums)
    transformed = out.reshape(2048, 2, 128).transpose(1, 0, 2).reshape(2, AMP_DEV)
    return transformed, checks


def solution(mesh):
    return jax.shard_map(
        per_device,
        mesh=mesh,
        in_specs=(P(None, AXES),),
        out_specs=(P(None, AXES), P()),
        check_vma=False,
    )
```

```python
import math

import jax
import jax.numpy as jnp
from jax import lax
from jax.experimental import pallas as pl
from jax.experimental.pallas import tpu as pltpu
from jax.sharding import PartitionSpec as P

MESH = pl.DeviceIdType.MESH
AXES = ("outer", "inner")
AMP_DEV = 262144
DEVICES = 256
TOTAL = AMP_DEV * DEVICES
WINDOW = 512
PITCH = 264
SPAN = 8 * PITCH


def reverse_bits(value, count):
    result = 0
    for bit in range(count):
        result = result + (value // 2**bit) % 2 * 2 ** (count - 1 - bit)
    return result


def scale_factor(squares):
    mean_square = squares / TOTAL
    return mean_square, lax.rsqrt(mean_square + 1e-06)


def exchange_kernel(
    x_hbm, placed_ref, late_ref, sums_ref,
    a_ref, high_ref, low_ref, bh_ref, bl_ref,
    send_ref, mid_a_ref, mid_b_ref, early_ref, zsum_ref, psum_ref,
    load_sem, send_sem, recv_sem, round_sem,
):
    loads = [
        [
            pltpu.make_async_copy(
                x_hbm.at[pl.ds(32 * top, 32), half],
                a_ref.at[half, reverse_bits(top, 3), pl.ds(0, 32)],
                load_sem.at[half, top],
            )
            for top in range(8)
        ]
        for half in range(2)
    ]
    for load in loads[0]:
        load.start()

    outer, inner = lax.axis_index("outer"), lax.axis_index("inner")
    y, c, x, z = outer // 2, outer % 2, inner // 8, inner % 8
    plane = outer * 4 + x
    z_slot, p_slot = reverse_bits(z, 3), reverse_bits(plane, 5)
    z_index = z % 2 * 4 + z // 2
    slot = z_slot * 32 + p_slot

    def z_peer(there):
        return (outer, x * 8 + there)

    def plane_peer(t):
        dx, dy, dc = t % 4, (t % 4 + t // 4) % 4, (t + t // 16) % 2
        there_outer, there_x = (y + dy) % 4 * 2 + (c + dc) % 2, (x + dx) % 4
        return (there_outer, there_x * 8 + z), there_outer * 4 + there_x

    barrier = pltpu.get_barrier_semaphore()
    for d in range(1, 8):
        pl.semaphore_signal(barrier, inc=1, device_id=z_peer((z + d) % 8), device_id_type=MESH)

    def greet(t, _):
        pl.semaphore_signal(barrier, inc=1, device_id=plane_peer(t)[0], device_id_type=MESH)
        return 0

    @pl.when(z == 0)
    def _():
        lax.fori_loop(1, 32, greet, 0)

    lane = lax.broadcasted_iota(jnp.int32, (128, 128), 1)
    row = lax.broadcasted_iota(jnp.int32, (128, 128), 0)
    frequency = (row & 31) * 4 + (row >> 5)
    angle = ((frequency * lane) & 127).astype(jnp.float32) * (2.0 * math.pi / 128)
    for value, places in (
        (jnp.cos(angle) * WINDOW**-0.5, ((0, 0, 1.0), (1, 1, 1.0))),
        (jnp.sin(angle) * WINDOW**-0.5, ((1, 0, 1.0), (0, 1, -1.0))),
    ):
        high = value.astype(jnp.bfloat16)
        low = (value - high.astype(jnp.float32)).astype(jnp.bfloat16)
        for i, j, sign in places:
            high_ref[128 * i : 128 * i + 128, 128 * j : 128 * j + 128] = high * jnp.bfloat16(sign)
            low_ref[128 * i : 128 * i + 128, 128 * j : 128 * j + 128] = low * jnp.bfloat16(sign)
    lane = lax.broadcasted_iota(jnp.int32, (16, 128), 1)
    twiddles = []
    for g in (1, 2, 3):
        angle = (lane * g).astype(jnp.float32) * (2.0 * math.pi / WINDOW)
        twiddles.append((jnp.cos(angle), jnp.sin(angle)))

    step = 2.0 * math.pi * 2048 / TOTAL
    cos_step, sin_step = math.cos(step), math.sin(step)
    a_rows = a_ref.reshape(2 * SPAN, 128)
    zero = jnp.zeros((8, 128), jnp.float32)

    def spread_half(half):
        for load in loads[half]:
            load.wait()
        if half == 0:
            for load in loads[1]:
                load.start()

        def spread(h, _):
            middle = reverse_bits(h, 4)
            parts = [
                [
                    a_rows[pl.ds(half * SPAN + (middle + 16 * b) * 8 + q, 8, stride=PITCH), :]
                    for q in range(8)
                ]
                for b in range(2)
            ]
            v = [jnp.concatenate([parts[0][q], parts[1][q]], 0) for q in range(8)]
            real, imag = v[0::2], v[1::2]
            s02r, s02i = real[0] + real[2], imag[0] + imag[2]
            d02r, d02i = real[0] - real[2], imag[0] - imag[2]
            s13r, s13i = real[1] + real[3], imag[1] + imag[3]
            d13r, d13i = real[1] - real[3], imag[1] - imag[3]
            u = [
                (s02r + s13r, s02i + s13i),
                (d02r - d13i, d02i + d13r),
                (s02r - s13r, s02i - s13i),
                (d02r + d13i, d02i - d13r),
            ]
            rows = pl.ds(pl.multiple_of(h * 16, 16), 16)
            for g in range(4):
                ur, ui = u[g]
                if g:
                    cosine, sine = twiddles[g - 1]
                    ur, ui = ur * cosine - ui * sine, ur * sine + ui * cosine
                for s, value in ((0, ur), (1, ui)):
                    high = value.astype(jnp.bfloat16)
                    low = (value - high.astype(jnp.float32)).astype(jnp.bfloat16)
                    bh_ref[g, rows, 128 * s : 128 * s + 128] = high
                    bl_ref[g, rows, 128 * s : 128 * s + 128] = low
            return 0

        lax.fori_loop(0, 16, spread, 0)

    def sums_half(half, squares):
        def add(turn, carry):
            squares, phase_real, phase_imag = carry
            middle = reverse_bits(15 - turn, 4)
            for b in (1, 0):
                part = [
                    a_rows[pl.ds(half * SPAN + (middle + 16 * b) * 8 + q, 8, stride=PITCH), :]
                    for q in range(8)
                ]
                phase_real, phase_imag = (
                    phase_real * cos_step + phase_imag * sin_step + part[0],
                    phase_imag * cos_step - phase_real * sin_step + part[1],
                )
                for q in range(8):
                    squares = squares + part[q] * part[q]
            return squares, phase_real, phase_imag

        return lax.fori_loop(0, 16, add, (squares, zero, zero))

    def transform(half, first):
        for f in range(2):
            bh, bl = bh_ref[first + f], bl_ref[first + f]
            dims = (((1,), (1,)), ((), ()))
            out = (
                lax.dot_general(high_ref[...], bh, dims, preferred_element_type=jnp.float32)
                + lax.dot_general(high_ref[...], bl, dims, preferred_element_type=jnp.float32)
                + lax.dot_general(low_ref[...], bh, dims, preferred_element_type=jnp.float32)
            )
            for k in range(2):
                for s in range(2):
                    place = pl.ds(first // 2 * 1024 + f * 4 + k * 2 + s, 128, stride=8)
                    send_ref[half, place, :] = out[128 * s : 128 * s + 128, 128 * k : 128 * k + 128]

    def copy(peer, source, target, number):
        return pltpu.make_async_remote_copy(
            src_ref=source,
            dst_ref=target,
            send_sem=send_sem.at[number],
            recv_sem=recv_sem.at[number],
            device_id=peer,
            device_id_type=MESH,
        )

    def finish_recv(ref, number):
        copy(z_peer((z + 1) % 8), ref, ref, number).wait_recv()

    def finish_send(ref, number):
        copy(z_peer((z + 1) % 8), ref, ref, number).wait_send()

    early_send = send_ref.reshape(2, 8, 32, 8, 128).at[0]
    late_send = send_ref.reshape(2, 2, 4, 32, 8, 128).at[1]

    spread_half(0)
    def early_z(there):
        copy(z_peer(there), early_send.at[there % 2 * 4 + there // 2], mid_a_ref.at[z_slot], 1).start()

    def early_sends(odd):
        @pl.when((z + odd) % 2 == 0)
        def _():
            for d in (4, 2, 6):
                early_z((z + d) % 8)

        @pl.when((z + odd) % 2 == 1)
        def _():
            for d in (3, 5, 1, 7):
                early_z((z + d) % 8)

    transform(0, 0)
    pl.semaphore_wait(barrier, 7 + jnp.where(z == 0, 31, 0))
    early_sends(0)
    transform(0, 2)
    early_sends(1)

    def line_ready(t, _):
        pl.semaphore_signal(round_sem.at[0], inc=1, device_id=plane_peer(t)[0], device_id_type=MESH)
        return 0

    @pl.when(z == 0)
    def _():
        lax.fori_loop(1, 32, line_ready, 0)

    spread_half(1)
    transform(1, 0)
    transform(1, 2)
    squares, phase_real_0, phase_imag_0 = sums_half(0, zero)
    squares, phase_real_1, phase_imag_1 = sums_half(1, squares)

    column = lax.broadcasted_iota(jnp.int32, (8, 128), 1)
    sub = lax.broadcasted_iota(jnp.int32, (8, 128), 0)
    turned_real, turned_imag = zero, zero
    for half, phase_real, phase_imag in ((0, phase_real_0, phase_imag_0), (1, phase_real_1, phase_imag_1)):
        angle = (half * 65536 + sub * 256 + slot).astype(jnp.float32) * (2.0 * math.pi / TOTAL)
        cosine, sine = jnp.cos(angle), jnp.sin(angle)
        turned_real = turned_real + (phase_real * cosine + phase_imag * sine)
        turned_imag = turned_imag + (phase_imag * cosine - phase_real * sine)
    lane = lax.broadcasted_iota(jnp.int32, (1, 128), 1)
    row = jnp.zeros((1, 128), jnp.float32)
    for i, value in enumerate((
        squares, jnp.where(column == 1, turned_real, 0.0), jnp.where(column == 1, turned_imag, 0.0),
    )):
        summed = jnp.sum(jnp.sum(value, 0, keepdims=True), 1, keepdims=True)
        row = jnp.where(lane == i, summed, row)
    psum_ref[plane] = row

    @pl.when(z == 0)
    def _():
        pl.semaphore_wait(round_sem.at[0], 31)
        for there in range(1, 8):
            pl.semaphore_signal(round_sem.at[1], inc=1, device_id=z_peer(there), device_id_type=MESH)

    @pl.when(z != 0)
    def _():
        pl.semaphore_wait(round_sem.at[1], 1)

    def plane_bulk(source, target, number):
        def body(t, _):
            peer, there = plane_peer(t)
            copy(peer, source.at[:, there], target.at[:, p_slot], number).start()
            return 0

        lax.fori_loop(1, 32, body, 0)

    def plane_sums(t, _):
        copy(plane_peer(t)[0], psum_ref.at[plane], psum_ref.at[plane], 3).start()
        return 0

    lax.fori_loop(1, 32, plane_sums, 0)

    def late_bulk(part):
        def body(t, _):
            peer, there = plane_peer(t)
            source = late_send.at[:, pl.ds(2 * part, 2), there]
            copy(peer, source, mid_b_ref.at[:, pl.ds(2 * part, 2), p_slot], 2 + 4 * part).start()
            return 0

        lax.fori_loop(1, 32, body, 0)

    late_bulk(0)
    late_bulk(1)
    mid_a_ref[z_slot] = early_send[z_index]
    for i in range(8):
        mid_b_ref[i // 4, i % 4, p_slot] = late_send[i // 4, i % 4, plane]

    finish_recv(psum_ref.at[pl.ds(0, 31)], 3)
    total = psum_ref[0]
    for i in range(1, 32):
        total = total + psum_ref[i]
    zsum_ref[z] = total
    for d in range(1, 8):
        copy(z_peer((z + d) % 8), zsum_ref.at[z], zsum_ref.at[z], 0).start()

    def late_z(there):
        copy(z_peer(there), mid_b_ref.at[there % 2, there // 2], late_ref.at[z_slot], 4).start()

    for part in range(2):
        finish_recv(mid_b_ref.at[:, pl.ds(0, 2), pl.ds(0, 31)], 2 + 4 * part)
        for there in (0, 1, 2, 3, 7, 4, 6, 5)[4 * part : 4 * part + 4]:
            pl.when(there != z)(lambda there=there: late_z(there))

    late_ref[z_slot] = mid_b_ref[z % 2, z // 2]

    finish_recv(mid_a_ref.at[pl.ds(0, 7)], 1)
    plane_bulk(mid_a_ref, early_ref, 5)
    for i in range(8):
        early_ref[i, p_slot] = mid_a_ref[i, plane]

    finish_recv(zsum_ref.at[pl.ds(0, 7)], 0)
    total = zsum_ref[0]
    for i in range(1, 8):
        total = total + zsum_ref[i]
    sums_ref[...] = total
    factor = scale_factor(total[:, 0:1])[1]

    finish_recv(early_ref.at[:, pl.ds(0, 31)], 5)
    place_rows(early_ref.reshape(2048, 128), placed_ref, factor)

    finish_recv(late_ref.at[pl.ds(0, 7)], 4)
    finish_send(zsum_ref.at[pl.ds(0, 7)], 0)
    finish_send(mid_a_ref.at[pl.ds(0, 7)], 1)
    finish_send(mid_b_ref.at[:, pl.ds(0, 2), pl.ds(0, 31)], 2)
    finish_send(mid_b_ref.at[:, pl.ds(0, 2), pl.ds(0, 31)], 6)
    finish_send(psum_ref.at[pl.ds(0, 31)], 3)
    finish_send(late_ref.at[pl.ds(0, 7)], 4)
    finish_send(early_ref.at[:, pl.ds(0, 31)], 5)


def place_rows(source, target, factor):
    def body(part, _):
        place_part(source, target, factor, part)
        return 0

    lax.fori_loop(0, 4, body, 0)


def place_part(source, target, factor, part):
    for s in range(2):
        for d in range(2):
            block = source[pl.ds(d * 1024 + part * 2 + s, 128, stride=8), :]
            target[pl.ds(part * 512 + d * 2 + s, 128, stride=4), :] = block.T * factor


def place_kernel(placed_ref, late_ref, sums_ref, out_hbm, checks_hbm, buffer_ref, checks_ref, sems):
    copies = []

    def move(source, first, size, number):
        copies.append(pltpu.make_async_copy(source, out_hbm.at[pl.ds(first, size)], sems.at[number]))
        copies[-1].start()

    for f in range(2):
        move(placed_ref.at[pl.ds(f * 1024, 1024)], f * 2048, 1024, f)
    sums = sums_ref[...]
    mean_square, factor = scale_factor(sums[:, 0:1])
    scale = factor * (math.sqrt(WINDOW) / math.sqrt(TOTAL))
    checks_ref[0] = mean_square[0, 0]
    for i in (1, 2):
        checks_ref[i] = (sums[:, i : i + 1] * scale)[0, 0]
    copies.append(pltpu.make_async_copy(checks_ref, checks_hbm, sems.at[6]))
    copies[-1].start()
    for part in range(4):
        place_part(late_ref, buffer_ref, factor, part)
        first = part // 2 * 2048 + 1024 + part % 2 * 512
        move(buffer_ref.at[pl.ds(part * 512, 512)], first, 512, 2 + part)
    for moved in copies:
        moved.wait()


def per_device(amplitudes):
    rows = amplitudes.reshape(2, 2048, 128).transpose(1, 0, 2).reshape(256, 2, 8, 128)
    vmem = pl.BlockSpec(memory_space=pltpu.VMEM)
    hbm = pl.BlockSpec(memory_space=pltpu.HBM)
    f32, bf16 = jnp.float32, jnp.bfloat16
    placed, late, sums = pl.pallas_call(
        exchange_kernel,
        out_shape=(
            jax.ShapeDtypeStruct((2048, 128), f32),
            jax.ShapeDtypeStruct((8, 32, 8, 128), f32),
            jax.ShapeDtypeStruct((1, 128), f32),
        ),
        in_specs=[hbm],
        out_specs=(vmem, vmem, vmem),
        scratch_shapes=[
            pltpu.VMEM((2, 8, 33, 8, 128), f32),
            pltpu.VMEM((256, 256), bf16),
            pltpu.VMEM((256, 256), bf16),
            pltpu.VMEM((4, 256, 256), bf16),
            pltpu.VMEM((4, 256, 256), bf16),
            pltpu.VMEM((2, 2048, 128), f32),
            pltpu.VMEM((8, 32, 8, 128), f32),
            pltpu.VMEM((2, 4, 32, 8, 128), f32),
            pltpu.VMEM((8, 32, 8, 128), f32),
            pltpu.VMEM((8, 1, 128), f32),
            pltpu.VMEM((32, 1, 128), f32),
            pltpu.SemaphoreType.DMA((2, 8)),
            pltpu.SemaphoreType.DMA((7,)),
            pltpu.SemaphoreType.DMA((7,)),
            pltpu.SemaphoreType.REGULAR((2,)),
        ],
        compiler_params=pltpu.CompilerParams(
            collective_id=1, has_side_effects=True, vmem_limit_bytes=51 * 1024 * 1024
        ),
    )(rows)
    out, checks = pl.pallas_call(
        place_kernel,
        out_shape=(
            jax.ShapeDtypeStruct((4096, 128), f32),
            jax.ShapeDtypeStruct((3,), f32),
        ),
        in_specs=[vmem, vmem, vmem],
        out_specs=(hbm, hbm),
        scratch_shapes=[
            pltpu.VMEM((2048, 128), f32),
            pltpu.SMEM((3,), f32),
            pltpu.SemaphoreType.DMA((7,)),
        ],
        compiler_params=pltpu.CompilerParams(vmem_limit_bytes=16 * 1024 * 1024),
    )(placed, late.reshape(2048, 128), sums)
    transformed = out.reshape(2048, 2, 128).transpose(1, 0, 2).reshape(2, AMP_DEV)
    return transformed, checks


def solution(mesh):
    return jax.shard_map(
        per_device,
        mesh=mesh,
        in_specs=(P(None, AXES),),
        out_specs=(P(None, AXES), P()),
        check_vma=False,
    )
```

```python
import math

import jax
import jax.numpy as jnp
from jax import lax
from jax.experimental import pallas as pl
from jax.experimental.pallas import tpu as pltpu
from jax.sharding import PartitionSpec as P

MESH = pl.DeviceIdType.MESH
AXES = ("outer", "inner")
AMP_DEV = 262144
DEVICES = 256
TOTAL = AMP_DEV * DEVICES
WINDOW = 512
PITCH = 264
SPAN = 8 * PITCH


def reverse_bits(value, count):
    result = 0
    for bit in range(count):
        result = result + (value // 2**bit) % 2 * 2 ** (count - 1 - bit)
    return result


def scale_factor(squares):
    mean_square = squares / TOTAL
    return mean_square, lax.rsqrt(mean_square + 1e-06)


def exchange_kernel(
    x_hbm, placed_ref, late_ref, sums_ref,
    a_ref, high_ref, low_ref, bh_ref, bl_ref,
    send_ref, mid_a_ref, mid_b_ref, early_ref, zsum_ref, psum_ref,
    load_sem, send_sem, recv_sem, round_sem,
):
    loads = [
        [
            pltpu.make_async_copy(
                x_hbm.at[pl.ds(32 * top, 32), half],
                a_ref.at[half, reverse_bits(top, 3), pl.ds(0, 32)],
                load_sem.at[half, top],
            )
            for top in range(8)
        ]
        for half in range(2)
    ]

    outer, inner = lax.axis_index("outer"), lax.axis_index("inner")
    y, c, x, z = outer // 2, outer % 2, inner // 8, inner % 8
    plane = outer * 4 + x
    z_slot, p_slot = reverse_bits(z, 3), reverse_bits(plane, 5)
    z_index = z % 2 * 4 + z // 2
    slot = z_slot * 32 + p_slot

    def z_peer(there):
        return (outer, x * 8 + there)

    def plane_peer(t):
        dx, dy, dc = t % 4, (t % 4 + t // 4) % 4, (t + t // 16) % 2
        there_outer, there_x = (y + dy) % 4 * 2 + (c + dc) % 2, (x + dx) % 4
        return (there_outer, there_x * 8 + z), there_outer * 4 + there_x

    barrier = pltpu.get_barrier_semaphore()
    for d in (4, 3, 5, 2, 6, 1, 7):
        pl.semaphore_signal(barrier, inc=1, device_id=z_peer((z + d) % 8), device_id_type=MESH)
    for load in loads[0]:
        load.start()

    def greet(t, _):
        pl.semaphore_signal(barrier, inc=1, device_id=plane_peer(t)[0], device_id_type=MESH)
        return 0

    @pl.when(z == 0)
    def _():
        lax.fori_loop(1, 32, greet, 0)

    lane = lax.broadcasted_iota(jnp.int32, (128, 128), 1)
    row = lax.broadcasted_iota(jnp.int32, (128, 128), 0)
    frequency = (row & 31) * 4 + (row >> 5)
    angle = ((frequency * lane) & 127).astype(jnp.float32) * (2.0 * math.pi / 128)
    for value, places in (
        (jnp.cos(angle) * WINDOW**-0.5, ((0, 0, 1.0), (1, 1, 1.0))),
        (jnp.sin(angle) * WINDOW**-0.5, ((1, 0, 1.0), (0, 1, -1.0))),
    ):
        high = value.astype(jnp.bfloat16)
        low = (value - high.astype(jnp.float32)).astype(jnp.bfloat16)
        for i, j, sign in places:
            high_ref[128 * i : 128 * i + 128, 128 * j : 128 * j + 128] = high * jnp.bfloat16(sign)
            low_ref[128 * i : 128 * i + 128, 128 * j : 128 * j + 128] = low * jnp.bfloat16(sign)
    lane = lax.broadcasted_iota(jnp.int32, (16, 128), 1)
    twiddles = []
    for g in (1, 2, 3):
        angle = (lane * g).astype(jnp.float32) * (2.0 * math.pi / WINDOW)
        twiddles.append((jnp.cos(angle), jnp.sin(angle)))

    step = 2.0 * math.pi * 2048 / TOTAL
    cos_step, sin_step = math.cos(step), math.sin(step)
    a_rows = a_ref.reshape(2 * SPAN, 128)
    zero = jnp.zeros((8, 128), jnp.float32)

    def spread_half(half):
        for load in loads[half]:
            load.wait()
        if half == 0:
            for load in loads[1]:
                load.start()

        def spread(h, _):
            middle = reverse_bits(h, 4)
            parts = [
                [
                    a_rows[pl.ds(half * SPAN + (middle + 16 * b) * 8 + q, 8, stride=PITCH), :]
                    for q in range(8)
                ]
                for b in range(2)
            ]
            v = [jnp.concatenate([parts[0][q], parts[1][q]], 0) for q in range(8)]
            real, imag = v[0::2], v[1::2]
            s02r, s02i = real[0] + real[2], imag[0] + imag[2]
            d02r, d02i = real[0] - real[2], imag[0] - imag[2]
            s13r, s13i = real[1] + real[3], imag[1] + imag[3]
            d13r, d13i = real[1] - real[3], imag[1] - imag[3]
            u = [
                (s02r + s13r, s02i + s13i),
                (d02r - d13i, d02i + d13r),
                (s02r - s13r, s02i - s13i),
                (d02r + d13i, d02i - d13r),
            ]
            rows = pl.ds(pl.multiple_of(h * 16, 16), 16)
            for g in range(4):
                ur, ui = u[g]
                if g:
                    cosine, sine = twiddles[g - 1]
                    ur, ui = ur * cosine - ui * sine, ur * sine + ui * cosine
                for s, value in ((0, ur), (1, ui)):
                    high = value.astype(jnp.bfloat16)
                    low = (value - high.astype(jnp.float32)).astype(jnp.bfloat16)
                    bh_ref[g, rows, 128 * s : 128 * s + 128] = high
                    bl_ref[g, rows, 128 * s : 128 * s + 128] = low
            return 0

        lax.fori_loop(0, 16, spread, 0)

    def sums_half(half, squares):
        def add(turn, carry):
            squares, phase_real, phase_imag = carry
            middle = reverse_bits(15 - turn, 4)
            for b in (1, 0):
                part = [
                    a_rows[pl.ds(half * SPAN + (middle + 16 * b) * 8 + q, 8, stride=PITCH), :]
                    for q in range(8)
                ]
                phase_real, phase_imag = (
                    phase_real * cos_step + phase_imag * sin_step + part[0],
                    phase_imag * cos_step - phase_real * sin_step + part[1],
                )
                for q in range(8):
                    squares = squares + part[q] * part[q]
            return squares, phase_real, phase_imag

        return lax.fori_loop(0, 16, add, (squares, zero, zero))

    def transform(half, first):
        for f in range(2):
            bh, bl = bh_ref[first + f], bl_ref[first + f]
            dims = (((1,), (1,)), ((), ()))
            out = (
                lax.dot_general(high_ref[...], bh, dims, preferred_element_type=jnp.float32)
                + lax.dot_general(high_ref[...], bl, dims, preferred_element_type=jnp.float32)
                + lax.dot_general(low_ref[...], bh, dims, preferred_element_type=jnp.float32)
            )
            for k in range(2):
                for s in range(2):
                    place = pl.ds(first // 2 * 1024 + f * 4 + k * 2 + s, 128, stride=8)
                    send_ref[half, place, :] = out[128 * s : 128 * s + 128, 128 * k : 128 * k + 128]

    def copy(peer, source, target, number):
        return pltpu.make_async_remote_copy(
            src_ref=source,
            dst_ref=target,
            send_sem=send_sem.at[number],
            recv_sem=recv_sem.at[number],
            device_id=peer,
            device_id_type=MESH,
        )

    def finish_recv(ref, number):
        copy(z_peer((z + 1) % 8), ref, ref, number).wait_recv()

    def finish_send(ref, number):
        copy(z_peer((z + 1) % 8), ref, ref, number).wait_send()

    early_send = send_ref.reshape(2, 8, 32, 8, 128).at[0]
    late_send = send_ref.reshape(2, 2, 4, 32, 8, 128).at[1]

    spread_half(0)
    def early_z(there):
        copy(z_peer(there), early_send.at[there % 2 * 4 + there // 2], mid_a_ref.at[z_slot], 1).start()

    def early_sends(odd):
        @pl.when((z + odd) % 2 == 0)
        def _():
            for d in (4, 2, 6):
                early_z((z + d) % 8)

        @pl.when((z + odd) % 2 == 1)
        def _():
            for d in (3, 5, 1, 7):
                early_z((z + d) % 8)

    transform(0, 0)
    pl.semaphore_wait(barrier, 7 + jnp.where(z == 0, 31, 0))
    early_sends(0)
    transform(0, 2)
    early_sends(1)

    def line_ready(t, _):
        pl.semaphore_signal(round_sem.at[0], inc=1, device_id=plane_peer(t)[0], device_id_type=MESH)
        return 0

    @pl.when(z == 0)
    def _():
        lax.fori_loop(1, 32, line_ready, 0)

    spread_half(1)
    transform(1, 0)
    transform(1, 2)
    squares, phase_real_0, phase_imag_0 = sums_half(0, zero)
    squares, phase_real_1, phase_imag_1 = sums_half(1, squares)

    column = lax.broadcasted_iota(jnp.int32, (8, 128), 1)
    sub = lax.broadcasted_iota(jnp.int32, (8, 128), 0)
    turned_real, turned_imag = zero, zero
    for half, phase_real, phase_imag in ((0, phase_real_0, phase_imag_0), (1, phase_real_1, phase_imag_1)):
        angle = (half * 65536 + sub * 256 + slot).astype(jnp.float32) * (2.0 * math.pi / TOTAL)
        cosine, sine = jnp.cos(angle), jnp.sin(angle)
        turned_real = turned_real + (phase_real * cosine + phase_imag * sine)
        turned_imag = turned_imag + (phase_imag * cosine - phase_real * sine)
    lane = lax.broadcasted_iota(jnp.int32, (1, 128), 1)
    row = jnp.zeros((1, 128), jnp.float32)
    for i, value in enumerate((
        squares, jnp.where(column == 1, turned_real, 0.0), jnp.where(column == 1, turned_imag, 0.0),
    )):
        summed = jnp.sum(jnp.sum(value, 0, keepdims=True), 1, keepdims=True)
        row = jnp.where(lane == i, summed, row)
    psum_ref[plane] = row

    @pl.when(z == 0)
    def _():
        pl.semaphore_wait(round_sem.at[0], 31)
        for there in range(1, 8):
            pl.semaphore_signal(round_sem.at[1], inc=1, device_id=z_peer(there), device_id_type=MESH)

    @pl.when(z != 0)
    def _():
        pl.semaphore_wait(round_sem.at[1], 1)

    def plane_bulk(source, target, number):
        def body(t, _):
            peer, there = plane_peer(t)
            copy(peer, source.at[:, there], target.at[:, p_slot], number).start()
            return 0

        lax.fori_loop(1, 32, body, 0)

    def plane_sums(t, _):
        copy(plane_peer(t)[0], psum_ref.at[plane], psum_ref.at[plane], 3).start()
        return 0

    lax.fori_loop(1, 32, plane_sums, 0)

    def late_bulk(part):
        def body(t, _):
            peer, there = plane_peer(t)
            source = late_send.at[:, pl.ds(2 * part, 2), there]
            copy(peer, source, mid_b_ref.at[:, pl.ds(2 * part, 2), p_slot], 2 + 4 * part).start()
            return 0

        lax.fori_loop(1, 32, body, 0)

    late_bulk(0)
    late_bulk(1)
    mid_a_ref[z_slot] = early_send[z_index]
    for i in range(8):
        mid_b_ref[i // 4, i % 4, p_slot] = late_send[i // 4, i % 4, plane]

    finish_recv(psum_ref.at[pl.ds(0, 31)], 3)
    total = psum_ref[0]
    for i in range(1, 32):
        total = total + psum_ref[i]
    zsum_ref[z] = total
    for d in range(1, 8):
        copy(z_peer((z + d) % 8), zsum_ref.at[z], zsum_ref.at[z], 0).start()

    def late_z(there):
        copy(z_peer(there), mid_b_ref.at[there % 2, there // 2], late_ref.at[z_slot], 4).start()

    for part in range(2):
        finish_recv(mid_b_ref.at[:, pl.ds(0, 2), pl.ds(0, 31)], 2 + 4 * part)
        for there in (0, 1, 2, 3, 7, 4, 6, 5)[4 * part : 4 * part + 4]:
            pl.when(there != z)(lambda there=there: late_z(there))

    late_ref[z_slot] = mid_b_ref[z % 2, z // 2]

    finish_recv(mid_a_ref.at[pl.ds(0, 7)], 1)
    plane_bulk(mid_a_ref, early_ref, 5)
    for i in range(8):
        early_ref[i, p_slot] = mid_a_ref[i, plane]

    finish_recv(zsum_ref.at[pl.ds(0, 7)], 0)
    total = zsum_ref[0]
    for i in range(1, 8):
        total = total + zsum_ref[i]
    sums_ref[...] = total
    factor = scale_factor(total[:, 0:1])[1]

    finish_recv(early_ref.at[:, pl.ds(0, 31)], 5)
    place_rows(early_ref.reshape(2048, 128), placed_ref, factor)

    finish_recv(late_ref.at[pl.ds(0, 7)], 4)
    finish_send(zsum_ref.at[pl.ds(0, 7)], 0)
    finish_send(mid_a_ref.at[pl.ds(0, 7)], 1)
    finish_send(mid_b_ref.at[:, pl.ds(0, 2), pl.ds(0, 31)], 2)
    finish_send(mid_b_ref.at[:, pl.ds(0, 2), pl.ds(0, 31)], 6)
    finish_send(psum_ref.at[pl.ds(0, 31)], 3)
    finish_send(late_ref.at[pl.ds(0, 7)], 4)
    finish_send(early_ref.at[:, pl.ds(0, 31)], 5)


def place_rows(source, target, factor):
    def body(part, _):
        place_part(source, target, factor, part)
        return 0

    lax.fori_loop(0, 4, body, 0)


def place_part(source, target, factor, part):
    for s in range(2):
        for d in range(2):
            block = source[pl.ds(d * 1024 + part * 2 + s, 128, stride=8), :]
            target[pl.ds(part * 512 + d * 2 + s, 128, stride=4), :] = block.T * factor


def place_kernel(placed_ref, late_ref, sums_ref, out_hbm, checks_hbm, buffer_ref, checks_ref, sems):
    copies = []

    def move(source, first, size, number):
        copies.append(pltpu.make_async_copy(source, out_hbm.at[pl.ds(first, size)], sems.at[number]))
        copies[-1].start()

    for f in range(2):
        move(placed_ref.at[pl.ds(f * 1024, 1024)], f * 2048, 1024, f)
    sums = sums_ref[...]
    mean_square, factor = scale_factor(sums[:, 0:1])
    scale = factor * (math.sqrt(WINDOW) / math.sqrt(TOTAL))
    checks_ref[0] = mean_square[0, 0]
    for i in (1, 2):
        checks_ref[i] = (sums[:, i : i + 1] * scale)[0, 0]
    copies.append(pltpu.make_async_copy(checks_ref, checks_hbm, sems.at[6]))
    copies[-1].start()
    for part in range(4):
        place_part(late_ref, buffer_ref, factor, part)
        first = part // 2 * 2048 + 1024 + part % 2 * 512
        move(buffer_ref.at[pl.ds(part * 512, 512)], first, 512, 2 + part)
    for moved in copies:
        moved.wait()


def per_device(amplitudes):
    rows = amplitudes.reshape(2, 2048, 128).transpose(1, 0, 2).reshape(256, 2, 8, 128)
    vmem = pl.BlockSpec(memory_space=pltpu.VMEM)
    hbm = pl.BlockSpec(memory_space=pltpu.HBM)
    f32, bf16 = jnp.float32, jnp.bfloat16
    placed, late, sums = pl.pallas_call(
        exchange_kernel,
        out_shape=(
            jax.ShapeDtypeStruct((2048, 128), f32),
            jax.ShapeDtypeStruct((8, 32, 8, 128), f32),
            jax.ShapeDtypeStruct((1, 128), f32),
        ),
        in_specs=[hbm],
        out_specs=(vmem, vmem, vmem),
        scratch_shapes=[
            pltpu.VMEM((2, 8, 33, 8, 128), f32),
            pltpu.VMEM((256, 256), bf16),
            pltpu.VMEM((256, 256), bf16),
            pltpu.VMEM((4, 256, 256), bf16),
            pltpu.VMEM((4, 256, 256), bf16),
            pltpu.VMEM((2, 2048, 128), f32),
            pltpu.VMEM((8, 32, 8, 128), f32),
            pltpu.VMEM((2, 4, 32, 8, 128), f32),
            pltpu.VMEM((8, 32, 8, 128), f32),
            pltpu.VMEM((8, 1, 128), f32),
            pltpu.VMEM((32, 1, 128), f32),
            pltpu.SemaphoreType.DMA((2, 8)),
            pltpu.SemaphoreType.DMA((7,)),
            pltpu.SemaphoreType.DMA((7,)),
            pltpu.SemaphoreType.REGULAR((2,)),
        ],
        compiler_params=pltpu.CompilerParams(
            collective_id=1, has_side_effects=True, vmem_limit_bytes=51 * 1024 * 1024
        ),
    )(rows)
    out, checks = pl.pallas_call(
        place_kernel,
        out_shape=(
            jax.ShapeDtypeStruct((4096, 128), f32),
            jax.ShapeDtypeStruct((3,), f32),
        ),
        in_specs=[vmem, vmem, vmem],
        out_specs=(hbm, hbm),
        scratch_shapes=[
            pltpu.VMEM((2048, 128), f32),
            pltpu.SMEM((3,), f32),
            pltpu.SemaphoreType.DMA((7,)),
        ],
        compiler_params=pltpu.CompilerParams(vmem_limit_bytes=16 * 1024 * 1024),
    )(placed, late.reshape(2048, 128), sums)
    transformed = out.reshape(2048, 2, 128).transpose(1, 0, 2).reshape(2, AMP_DEV)
    return transformed, checks


def solution(mesh):
    return jax.shard_map(
        per_device,
        mesh=mesh,
        in_specs=(P(None, AXES),),
        out_specs=(P(None, AXES), P()),
        check_vma=False,
    )
```
